128 devices in a mesh: wide: 8 (over z, x_hi), narrow: 4 (over y), depth: 4 (over x_lo, core).
Axes of the slice: x: 4 (x_hi: 2, x_lo: 2; x = x_hi * 2 + x_lo), y: 4, z: 4, core: 2. Of those that a mesh axis runs over, the one named last changes fastest.
Arguments:
- hidden_in: bfloat16 [2048, 4096], P(('wide', 'narrow'), 'depth'), may hold values from -36 to 36
- queries: bfloat16 [2048, 4096], P('wide', ('narrow', 'depth')), may hold values from -8 to 8
- lang_ids: int32 [2048], replicated, may hold values from 0 to 7
- owner_slot: int32 [8], replicated, may hold values from 0 to 7, each once
- enc_kv: bfloat16 [8, 2, 768, 4096], P('wide', None, None, ('narrow', 'depth')), may hold values from -7 to 7
- attn_proj: bfloat16 [4096, 4096], P(('narrow', 'depth')), may hold values from -0.09375 to 0.09375
- norm_gain: float32 [4096], replicated, may hold values from 0.25 to 1.75
- router_proj: float32 [4096, 4], replicated, may hold values from -0.09375 to 0.09375
- expert_ids: int32 [2048, 2], P('wide'), may hold values from 0 to 3, all different within a row; in each aligned block of 64 rows (0 to 63, 64 to 127, ...) at most 48 rows name the same one
- proj_in: bfloat16 [4, 4096, 5120], P('narrow', None, 'depth'), may hold values from -0.09375 to 0.09375
- proj_out: bfloat16 [4, 5120, 4096], P('narrow', 'depth'), may hold values from -0.078125 to 0.078125
Outputs:
- layer_out: bfloat16 [2048, 4096], P(('wide', 'narrow'), 'depth')
The draws below stay inside these ranges and needn't reach their ends.
Inputs may be any that keep to these rules, and one draw needn't show every extreme that they name: `owner_slot`: every slot once. `expert_ids`: each row names two different experts. Within each aligned block of 64 rows (the rows of one index of wide+narrow) no expert is named more than 48 times, a bound that some block reaches.
All inputs are finite; a program needn't handle non-finite values.
Results may differ from the reference program's by a relative error of at most 0.017.
Values may be sent and summed in bfloat16 or wider, within the bound.
No kernel may reach another device: no remote copies, remote signals or barrier semaphores. Data moves between devices by JAX's collectives and lax.ppermute only.
A program may use at most 128 MiB of HBM per device.

```python
import math
import jax
import jax.numpy as jnp
import numpy as np
from jax import lax

D = 4096
HEADS = 64
HEAD_DIM = 64
FF = 5120
ENC = 768
TOK_DEV = 64
EXPERTS = 4
LANGS = 8
BATCH = 2048
CAP = 48


def draw_queries(key, part):
    base_draw = 1.5 * jax.random.truncated_normal(jax.random.fold_in(key, 1), -4.0, 4.0, (BATCH, HEADS * HEAD_DIM), jnp.float32)
    return base_draw.astype(jnp.bfloat16)


def draw_enc_kv(key, part):
    width_all = HEADS * HEAD_DIM
    offset = jax.random.truncated_normal(jax.random.fold_in(key, 2), -3.0, 3.0, (LANGS, 1, width_all), jnp.float32)
    noise_part = jax.random.truncated_normal(jax.random.fold_in(key, 3), -4.0, 4.0, (LANGS, ENC, width_all), jnp.float32)
    value_part = offset + noise_part
    key_part = jax.random.truncated_normal(jax.random.fold_in(key, 4), -4.0, 4.0, (LANGS, ENC, width_all), jnp.float32)
    return jnp.stack([key_part, value_part], axis=1).astype(jnp.bfloat16)


def draw_hidden_in(key, part):
    base_draw = jax.random.truncated_normal(jax.random.fold_in(key, 5), -4.0, 4.0, (BATCH, D), jnp.float32)
    return base_draw.astype(jnp.bfloat16)


def plant(drawn, key, least, largest):
    longest = drawn.shape.index(max(drawn.shape))
    spots = []
    for shift in (0, 1):
        where = [jax.random.randint(jax.random.fold_in(key, axis), (), 0, length) for axis, length in enumerate(drawn.shape)]
        where[longest] = (where[longest] + shift) % drawn.shape[longest]
        spots.append(tuple(where))
    return drawn.at[spots[0]].set(least).at[spots[1]].set(largest)


def shard_levels(key, shape, shards, least, largest):
    def one(dim, shards_of):
        draws = jax.random.uniform(jax.random.fold_in(jax.random.fold_in(key, 6), dim), (shards_of,), jnp.float32, least / len(shards), largest / len(shards))
        return jnp.repeat(jnp.exp(draws), shape[dim] // shards_of).reshape((-1,) + (1,) * (len(shape) - dim - 1))

    level = one(*shards[0])
    for cut in shards[1:]:
        level = level * one(*cut)
    return level


def cumulative_ranks(amount, skew):
    loads = [(1 << 20) // math.isqrt(standing ** skew) + 1 for standing in range(1, amount + 1)]
    deviation = 1 + sum(loads) // (1 << 30)
    return np.cumsum(np.array([max(1, weight // deviation) for weight in loads]))


def ranked(stream_key, dims, count, slope):
    grid = cumulative_ranks(count, slope)
    ticket = jax.random.randint(jax.random.fold_in(stream_key, 1), dims, 0, int(grid[count - 1]))
    grade = jnp.searchsorted(jnp.asarray(grid, jnp.int32), ticket, side="right")
    return jax.random.permutation(jax.random.fold_in(stream_key, 2), count)[grade].astype(jnp.int32)


def shared_out(key, own, number, rows, number_of, top, limit, lean):
    order = jax.random.permutation(key, number_of)
    heavy_load, ordinary = portions_of(number_of, rows * top, limit, lean, True), portions_of(number_of, rows * top, limit, lean, False)
    places = jnp.arange(number_of)

    def named(tallies, rotation):
        used = int((tallies > 0).sum())
        fixed = max(1, used // 4)
        moved = fixed + (places - fixed + rotation * (used - fixed)) % max(1, number_of - fixed)
        return jnp.zeros((number_of,), jnp.int32).at[order[jnp.where(places < fixed, places, moved)]].set(jnp.asarray(tallies, jnp.int32))

    tallies = jnp.where(number % 4 == 0, named(heavy_load, number // 4), named(ordinary, number - number // 4 - 1))
    mixed = jax.random.permutation(jax.random.fold_in(own, 3), number_of)
    source_of, receiver = mixed[0:number_of // 2 * 2:2], mixed[1:number_of // 2 * 2:2]
    margin = jnp.minimum(tallies[source_of] - 1, limit - tallies[receiver]) // 2
    margin = jnp.where((source_of == order[0]) | (receiver == order[0]) | (tallies[receiver] == 0), 0, jnp.maximum(margin, 0))
    moved = jax.random.randint(jax.random.fold_in(own, 4), (number_of // 2,), 0, 1 << 20) % (margin + 1)
    tallies = tallies.at[source_of].add(-moved).at[receiver].add(moved)
    items = jnp.searchsorted(jnp.cumsum(tallies), jnp.arange(rows * top), side="right").astype(jnp.int32)
    table = items.reshape(top, rows).T
    table = table[jax.random.permutation(jax.random.fold_in(own, 1), rows)]
    rotation = jax.random.randint(jax.random.fold_in(own, 2), (rows, 1), 0, top)
    return jnp.take_along_axis(table, (jnp.arange(top)[None, :] + rotation) % top, axis=1)


def portions_of(amount, total, most, slope, full):
    loads = [(1 << 20) // math.isqrt(grade ** slope) + 1 for grade in range(1, amount + 1)]
    largest = most if full else min(most, max(-(-total // amount), total * loads[0] // sum(loads)))
    least = 1 if total - largest >= amount - 1 else 0
    holding, spare = [largest] + [least] * (amount - 1), total - largest - least * (amount - 1)
    while spare > 0:
        free = [i for i in range(1, amount) if holding[i] < largest] or [i for i in range(1, amount) if holding[i] < most]
        whole, remaining = sum([loads[i] for i in free]), spare
        for i in free:
            more = min(most - holding[i], max(1, remaining * loads[i] // whole), spare)
            holding[i] = holding[i] + more
            spare = spare - more
    return np.array(holding)


def normal_values(key, shape, spread, reach, split=(), held_as=jnp.bfloat16):
    entries = spread * jax.random.normal(key, shape, jnp.float32)
    if split:
        entries = entries * shard_levels(key, shape, split, -0.22, 0.18)
    return jnp.clip(entries, -reach, reach).astype(held_as)


def setup_inputs(seed: int = 0) -> dict:
    streams_of = jax.random.split(jax.random.key(seed), 12)
    hidden_in = draw_hidden_in(jax.random.fold_in(streams_of[11], 71), 0)
    queries = draw_queries(jax.random.fold_in(streams_of[11], 71), 0)
    lang_ids = plant(ranked(streams_of[2], (BATCH,), LANGS, 2), jax.random.fold_in(streams_of[2], 3), 0, LANGS - 1).astype(jnp.int32)
    owner_slot = jax.random.permutation(streams_of[3], LANGS).astype(jnp.int32)
    enc_kv = draw_enc_kv(jax.random.fold_in(streams_of[11], 71), 0)
    attn_proj = normal_values(streams_of[5], (HEADS * HEAD_DIM, D), (HEADS * HEAD_DIM) ** -0.5, 0.09375, ((0, 16),))
    norm_gain = jnp.clip(1.0 + 0.15 * jax.random.normal(streams_of[6], (D,), jnp.float32), 0.25, 1.75)
    router_proj = normal_values(streams_of[7], (D, EXPERTS), D ** -0.5, 0.09375, (), jnp.float32)
    expert_ids_keys = jax.random.split(jax.random.fold_in(streams_of[8], 1), BATCH // TOK_DEV)
    expert_ids_turns = jax.random.permutation(jax.random.fold_in(streams_of[8], 3), BATCH // TOK_DEV)
    expert_ids = jax.vmap(lambda own, number: shared_out(jax.random.fold_in(streams_of[8], 2), own, number, TOK_DEV, EXPERTS, 2, CAP, 2))(expert_ids_keys, expert_ids_turns).reshape((BATCH, 2))
    proj_in = normal_values(streams_of[9], (EXPERTS, D, FF), D ** -0.5, 0.09375, ((0, 4), (2, 4)))
    proj_out = normal_values(streams_of[10], (EXPERTS, FF, D), FF ** -0.5, 0.078125, ((0, 4), (1, 4)))
    return {"hidden_in": hidden_in, "queries": queries, "lang_ids": lang_ids, "owner_slot": owner_slot, "enc_kv": enc_kv, "attn_proj": attn_proj, "norm_gain": norm_gain, "router_proj": router_proj, "expert_ids": expert_ids, "proj_in": proj_in, "proj_out": proj_out}


norm_eps = 1e-06

def reference(hidden_in, queries, lang_ids, owner_slot, enc_kv, attn_proj, norm_gain, router_proj, expert_ids, proj_in, proj_out):
    holder = owner_slot[lang_ids].astype(jnp.int32)
    block_rows = math.gcd(BATCH, 512)

    def attend(element):
        query_part, slot_tags = element
        query_rows = query_part.astype(jnp.float32).reshape(block_rows, HEADS, HEAD_DIM)

        def per_slot(running_sum, position):
            kv_pair = lax.dynamic_index_in_dim(enc_kv, position, 0, keepdims=False).astype(jnp.float32)
            key_rows = kv_pair[0].reshape(ENC, HEADS, HEAD_DIM)
            value_rows = kv_pair[1].reshape(ENC, HEADS, HEAD_DIM)
            scores = jnp.einsum('rhd,khd->rhk', query_rows, key_rows) * HEAD_DIM ** (-0.5)
            weights = jnp.exp(scores - lax.optimization_barrier(jnp.max(scores, axis=2, keepdims=True)))
            denominator = lax.optimization_barrier(jnp.sum(weights, axis=2))
            rounded = lax.optimization_barrier(weights.astype(jnp.bfloat16)).astype(jnp.float32)
            context = jnp.einsum('rhk,khd->rhd', rounded, value_rows) / denominator[:, :, None]
            return (running_sum + jnp.where((slot_tags == position)[:, None, None], context, 0.0), None)
        start_sum = jnp.zeros((block_rows, HEADS, HEAD_DIM), jnp.float32)
        running_sum, _ = lax.scan(per_slot, start_sum, jnp.arange(LANGS, dtype=jnp.int32))
        return running_sum.reshape(block_rows, HEADS * HEAD_DIM)
    context = lax.map(attend, (queries.reshape(BATCH // block_rows, block_rows, HEADS * HEAD_DIM), holder.reshape(BATCH // block_rows, block_rows)))
    context = context.reshape(BATCH, HEADS * HEAD_DIM).astype(jnp.bfloat16)
    attn_out = jnp.dot(context, attn_proj, preferred_element_type=jnp.float32)
    residual = (hidden_in.astype(jnp.float32) + attn_out).astype(jnp.bfloat16)
    resid_f32 = residual.astype(jnp.float32)
    inv_norm = lax.rsqrt(lax.optimization_barrier(jnp.mean(resid_f32 * resid_f32, axis=1)) + norm_eps)
    normed = (resid_f32 * inv_norm[:, None] * norm_gain[None, :]).astype(jnp.bfloat16)
    logits = jnp.dot(normed.astype(jnp.float32), router_proj, precision=lax.Precision.HIGHEST)
    pick_mask = expert_ids[:, :, None] == jnp.arange(EXPERTS, dtype=jnp.int32)[None, None, :]
    own_logit = lax.optimization_barrier(jnp.sum(jnp.where(pick_mask, logits[:, None, :], 0.0), axis=2))
    gates = jax.nn.sigmoid(own_logit - own_logit[:, ::-1])
    expert_weight = lax.optimization_barrier(jnp.sum(jnp.where(pick_mask, gates[:, :, None], 0.0), axis=1))

    def add_expert(running_sum, position):
        first_proj = lax.dynamic_index_in_dim(proj_in, position, 0, keepdims=False)
        second_proj = lax.dynamic_index_in_dim(proj_out, position, 0, keepdims=False)
        hidden_act = jnp.dot(normed, first_proj, preferred_element_type=jnp.float32)
        hidden_act = jax.nn.gelu(hidden_act, approximate=True).astype(jnp.bfloat16)
        expert_out = jnp.dot(hidden_act, second_proj, preferred_element_type=jnp.float32)
        expert_share = lax.optimization_barrier(jnp.sum(jnp.where(jnp.arange(EXPERTS, dtype=jnp.int32)[None, :] == position, expert_weight, 0.0), axis=1))
        return (running_sum + expert_share[:, None] * expert_out, None)
    start_total = jnp.zeros((BATCH, D), jnp.float32)
    moe_out, _ = lax.scan(add_expert, start_total, jnp.arange(EXPERTS, dtype=jnp.int32))
    return (resid_f32 + moe_out).astype(jnp.bfloat16)
```

```python
import functools

import jax
import jax.numpy as jnp
from jax import lax
from jax.experimental import pallas as pl
from jax.experimental.pallas import tpu as pltpu
from jax.sharding import PartitionSpec as P

HEAD_DIM = 64
CAP = 48
norm_eps = 1e-06
F32 = jnp.float32
BF16 = jnp.bfloat16
ROWS_BLOCK = 256
LIMIT = 60 * 1024 * 1024


def dot(a, b):
    return jnp.dot(a, b, preferred_element_type=F32)


def iota(shape, dim):
    return lax.broadcasted_iota(jnp.int32, shape, dim)


def one_hot(flags):
    return jnp.where(flags, 1.0, 0.0).astype(BF16)


def vmem(*shape_dtype):
    return pltpu.VMEM(*shape_dtype)


def attend_kernel(place, slot_of, lang_ref, q_ref, kt_ref, v_ref, out_ref, packed, attended):
    sources, rows, width = q_ref.shape
    heads = width // HEAD_DIM
    span = rows + 16
    wide_span = rows + 128
    langs = lang_ref[...]
    holder = jnp.zeros_like(langs)
    for lang in range(slot_of.shape[0]):
        holder = jnp.where(langs == lang, slot_of[lang], holder)
    mine = holder == place[0]
    upto = one_hot(iota((rows, rows), 0) <= iota((rows, rows), 1))
    within = dot(one_hot(mine), upto)
    counts = within[:, rows - 1 :]
    begins = [jnp.int32(0)]
    before = jnp.zeros((sources, 1), F32)
    for source in range(sources):
        count = counts[source : source + 1, :]
        before = before + jnp.where(iota((sources, 1), 0) > source, count, 0.0)
        begins.append(begins[-1] + jnp.sum(count).astype(jnp.int32))
    pos = jnp.where(mine, within - 1.0 + before, -1.0)
    pos_row = pos.astype(jnp.int32)
    pos_col = pos.T.astype(jnp.int32)
    packed[...] = jnp.zeros_like(packed)
    attended[...] = jnp.zeros_like(attended)
    for source in range(sources):
        at = pl.multiple_of((begins[source] // 16) * 16, 16)
        pick = one_hot(iota((span, rows), 0) + at == pos_row[source : source + 1, :])
        moved = dot(pick, q_ref[source]).astype(BF16)
        packed[pl.ds(at, span), :] += moved

    head_of = iota((1, width), 1) // HEAD_DIM

    def block(index, _):
        here = pl.ds(pl.multiple_of(index * ROWS_BLOCK, ROWS_BLOCK), ROWS_BLOCK)
        query = packed[here, :] * jnp.asarray(HEAD_DIM**-0.5, BF16)
        total = jnp.zeros((ROWS_BLOCK, width), F32)
        for head in range(heads):
            mine = head_of == head
            scores = dot(jnp.where(mine, query, jnp.zeros_like(query)), kt_ref[...])
            weights = jnp.exp(scores - jnp.max(scores, axis=1, keepdims=True))
            norm = jnp.sum(weights, axis=1, keepdims=True)
            taken = dot(weights.astype(BF16), v_ref[...])
            total = jnp.where(mine, taken / norm, total)
        attended[here, :] = total.astype(BF16)
        return 0

    lax.fori_loop(0, (begins[sources] + ROWS_BLOCK - 1) // ROWS_BLOCK, block, 0)
    for source in range(sources):
        at = pl.multiple_of((begins[source] // 16) * 16, 16)
        put = one_hot(iota((rows, wide_span), 1) + at == pos_col[:, source : source + 1])
        out_ref[source] = dot(put, attended[pl.ds(at, wide_span), :]).astype(BF16)


def attend(wide_at, owner_slot, langs, queries, keys_t, values):
    sources, rows, width = queries.shape
    capacity = sources * rows + 2 * ROWS_BLOCK
    in_vmem = pl.BlockSpec(memory_space=pltpu.VMEM)
    in_smem = pl.BlockSpec(memory_space=pltpu.SMEM)
    return pl.pallas_call(
        attend_kernel,
        out_shape=jax.ShapeDtypeStruct(queries.shape, BF16),
        in_specs=[in_smem] * 2 + [in_vmem] * 4,
        out_specs=in_vmem,
        scratch_shapes=[pltpu.VMEM((capacity, width), BF16)] * 2,
        cost_estimate=pl.CostEstimate(flops=10**9, bytes_accessed=4 * 10**6, transcendentals=10**6),
        compiler_params=pltpu.CompilerParams(vmem_limit_bytes=32 * 1024 * 1024),
        name="attend",
    )(wide_at, owner_slot, langs, queries, keys_t, values)


def project_kernel(place, *refs):
    parts = (len(refs) - 3) // 2
    ctx_refs, proj_refs = refs[:parts], refs[parts : 2 * parts]
    send_ref, keep_ref, full = refs[2 * parts :]
    rows = send_ref.shape[1]
    acc = dot(ctx_refs[0][...], proj_refs[0][...])
    for part in range(1, parts):
        acc = acc + dot(ctx_refs[part][...], proj_refs[part][...])
    full[...] = acc
    core = place[0]
    for far in range(2):
        gone = pl.multiple_of((far * 2 + 1 - core) * rows, rows)
        kept = pl.multiple_of((far * 2 + core) * rows, rows)
        send_ref[far] = full[pl.ds(gone, rows), :].astype(BF16)
        keep_ref[far] = full[pl.ds(kept, rows), :]


def project(core, contexts, projs):
    rows, width = contexts[0].shape
    cols = projs[0].shape[1]
    in_vmem = pl.BlockSpec(memory_space=pltpu.VMEM)
    return pl.pallas_call(
        project_kernel,
        out_shape=(
            jax.ShapeDtypeStruct((2, rows // 4, cols), BF16),
            jax.ShapeDtypeStruct((2, rows // 4, cols), F32),
        ),
        in_specs=[pl.BlockSpec(memory_space=pltpu.SMEM)] + [in_vmem] * (len(contexts) + len(projs)),
        out_specs=(in_vmem, in_vmem),
        scratch_shapes=[pltpu.VMEM((rows, cols), F32)],
        cost_estimate=pl.CostEstimate(flops=10**9, bytes_accessed=4 * 10**6, transcendentals=0),
        compiler_params=pltpu.CompilerParams(vmem_limit_bytes=24 * 1024 * 1024),
        name="project",
    )(core, *contexts, *projs)


def dispatch_kernel(near_ref, got_ref, hidden_ref, slot_ref, resid_ref, *box_refs):
    for far in range(2):
        summed = near_ref[far].astype(F32) + got_ref[far].astype(F32)
        residual = (hidden_ref[far].astype(F32) + summed).astype(BF16)
        resid_ref[far] = residual
        for step, box_ref in enumerate(box_refs):
            index = step * 2 + far
            pick = one_hot(iota((CAP, residual.shape[0]), 0) == slot_ref[index : index + 1, :])
            box_ref[far] = dot(pick, residual).astype(BF16)


def dispatch(near, got, hidden, slots):
    _, rows, cols = near.shape
    steps = slots.shape[0] // 2
    in_vmem = pl.BlockSpec(memory_space=pltpu.VMEM)
    return pl.pallas_call(
        dispatch_kernel,
        out_shape=(jax.ShapeDtypeStruct(near.shape, BF16),)
        + (jax.ShapeDtypeStruct((2, CAP, cols), BF16),) * steps,
        in_specs=[in_vmem] * 4,
        out_specs=(in_vmem,) * (1 + steps),
        cost_estimate=pl.CostEstimate(flops=10**8, bytes_accessed=2 * 10**6, transcendentals=0),
        compiler_params=pltpu.CompilerParams(vmem_limit_bytes=16 * 1024 * 1024),
        name="dispatch",
    )(near, got, hidden, slots)


def hold_kernel(from_ref, _, held_ref, sems):
    pieces = sems.shape[0]
    rows = from_ref.shape[0] // pieces
    copies = [
        pltpu.make_async_copy(
            from_ref.at[pl.ds(piece * rows, rows)], held_ref.at[pl.ds(piece * rows, rows)], sems.at[piece]
        )
        for piece in range(pieces)
    ]
    for copy in copies:
        copy.start()
    for copy in copies:
        copy.wait()


def hold(weight, after, grant):
    in_vmem = pl.BlockSpec(memory_space=pltpu.VMEM)
    return pl.pallas_call(
        hold_kernel,
        out_shape=jax.ShapeDtypeStruct(weight.shape, weight.dtype),
        in_specs=[pl.BlockSpec(memory_space=pltpu.HBM), in_vmem],
        out_specs=in_vmem,
        scratch_shapes=[pltpu.SemaphoreType.DMA((8,))],
        cost_estimate=pl.CostEstimate(flops=4 * 10**9, bytes_accessed=10**7, transcendentals=0),
        compiler_params=pltpu.CompilerParams(vmem_limit_bytes=grant * 1024 * 1024),
        name="hold",
    )(weight, after)


IN_COLS = 640
OUT_COLS = 1024


def expert_kernel(place, *refs):
    parts = 4
    row_refs = refs[: 2 * parts]
    gain_ref, router_ref, choose_ref, w_in, w_out, send_ref, keep_ref = refs[2 * parts : 2 * parts + 7]
    rows_all, hidden = refs[2 * parts + 7 :]
    narrow_at, core = place[0], place[1]
    features, hidden_units = w_in.shape
    _, slots, quarter = row_refs[0].shape
    blocks = [lax.rem(narrow_at + parts - step, parts) for step in range(parts)]

    for which, side in ((0, core), (1, 1 - core)):
        for far in range(2):
            squares = jnp.zeros((slots, 1), F32)
            for part in range(parts):
                rows = row_refs[which * parts + part][far].astype(F32)
                squares = squares + jnp.sum(rows * rows, axis=1, keepdims=True)
            inverse = lax.rsqrt(squares / features + norm_eps)
            at = pl.multiple_of((far * 2 + side) * slots, 16)
            for part in range(parts):
                rows = row_refs[which * parts + part][far].astype(F32)
                normed = rows * inverse * gain_ref[blocks[part]]
                rows_all[part, pl.ds(at, slots), :] = normed.astype(BF16)
    logits = dot(rows_all[0], router_ref[blocks[0]])
    for part in range(1, parts):
        logits = logits + dot(rows_all[part], router_ref[blocks[part]])
    differ = jnp.sum(logits * choose_ref[...], axis=1, keepdims=True)
    gate = 1.0 / (1.0 + jnp.exp(-differ))
    for step in range(hidden_units // IN_COLS):
        cols = slice(step * IN_COLS, (step + 1) * IN_COLS)
        acc = None
        for part in range(parts):
            at = pl.multiple_of(blocks[part] * quarter, quarter)
            term = dot(rows_all[part], w_in[pl.ds(at, quarter), cols])
            acc = term if acc is None else acc + term
        hidden[:, cols] = jax.nn.gelu(acc, approximate=True).astype(BF16)
    for kept in range(2):
        side = core if kept else 1 - core
        for far in range(2):
            for step in range(quarter // OUT_COLS):
                at = pl.multiple_of((far * 2 + side) * quarter + step * OUT_COLS, OUT_COLS)
                acc = dot(hidden[...], w_out[:, pl.ds(at, OUT_COLS)]) * gate
                cols = slice(step * OUT_COLS, (step + 1) * OUT_COLS)
                if kept:
                    keep_ref[far, :, cols] = acc
                else:
                    send_ref[far, :, cols] = acc.astype(BF16)


def expert(place, own, other, gain, router, choose, w_in, w_out):
    _, slots, quarter = own[0].shape
    parts = len(own)
    rows = 4 * slots
    features, units = w_in.shape
    in_vmem = pl.BlockSpec(memory_space=pltpu.VMEM)
    return pl.pallas_call(
        expert_kernel,
        out_shape=(
            jax.ShapeDtypeStruct((2, rows, quarter), BF16),
            jax.ShapeDtypeStruct((2, rows, quarter), F32),
        ),
        in_specs=[pl.BlockSpec(memory_space=pltpu.SMEM)]
        + [in_vmem] * (2 * parts + 5),
        out_specs=(in_vmem, in_vmem),
        scratch_shapes=[
            pltpu.VMEM((parts, rows, quarter), BF16),
            pltpu.VMEM((rows, units), BF16),
        ],
        cost_estimate=pl.CostEstimate(flops=4 * 10**9, bytes_accessed=24 * 10**6, transcendentals=10**5),
        compiler_params=pltpu.CompilerParams(vmem_limit_bytes=12 * 1024 * 1024),
        name="expert",
    )(place, *own, *other, gain, router, choose, w_in, w_out)


def share_kernel(place, keep_ref, got_ref, *box_refs):
    slots = box_refs[0].shape[1]
    for step, box_ref in enumerate(box_refs):
        block = lax.rem(place[0] + step, len(box_refs))
        at = pl.ds(pl.multiple_of(block * slots, 16), slots)
        for far in range(2):
            box_ref[far] = (keep_ref[far, at, :] + got_ref[far, at, :].astype(F32)).astype(BF16)


def share(place, keep, got, peers):
    _, rows, cols = keep.shape
    in_vmem = pl.BlockSpec(memory_space=pltpu.VMEM)
    return pl.pallas_call(
        share_kernel,
        out_shape=(jax.ShapeDtypeStruct((2, rows // peers, cols), BF16),) * peers,
        in_specs=[pl.BlockSpec(memory_space=pltpu.SMEM), in_vmem, in_vmem],
        out_specs=(in_vmem,) * peers,
        cost_estimate=pl.CostEstimate(flops=10**7, bytes_accessed=4 * 10**6, transcendentals=0),
        compiler_params=pltpu.CompilerParams(vmem_limit_bytes=16 * 1024 * 1024),
        name="share",
    )(place, keep, got)


def combine_kernel(place, slot_ref, resid_ref, *refs):
    box_refs, (send_ref, keep_ref, both) = refs[:-3], refs[-3:]
    tokens = slot_ref.shape[1]
    for far in range(2):
        acc = jnp.zeros(both.shape[1:], F32)
        for step, box_ref in enumerate(box_refs):
            pick = one_hot(iota((tokens, CAP), 1) == slot_ref[step])
            acc = acc + dot(pick, box_ref[far])
        both[far] = acc
    send_ref[...] = both[1 - place[0]].astype(BF16)
    keep_ref[...] = both[place[0]] + resid_ref[...].astype(F32)


def combine(place, slots, resid, boxes):
    in_vmem = pl.BlockSpec(memory_space=pltpu.VMEM)
    return pl.pallas_call(
        combine_kernel,
        out_shape=(
            jax.ShapeDtypeStruct(resid.shape, BF16),
            jax.ShapeDtypeStruct(resid.shape, F32),
        ),
        in_specs=[pl.BlockSpec(memory_space=pltpu.SMEM)] + [in_vmem] * (2 + len(boxes)),
        out_specs=(in_vmem, in_vmem),
        scratch_shapes=[pltpu.VMEM((2, *resid.shape), F32)],
        cost_estimate=pl.CostEstimate(flops=10**8, bytes_accessed=2 * 10**6, transcendentals=0),
        compiler_params=pltpu.CompilerParams(vmem_limit_bytes=16 * 1024 * 1024),
        name="combine",
    )(place, slots, resid, *boxes)


def ring(count, step):
    return [(i, (i + step) % count) for i in range(count)]


def pick_at(values, index, axis=0):
    return lax.dynamic_index_in_dim(values, index, axis, keepdims=False)


def to_all(value, axis):
    peers = lax.axis_size(axis)
    return lax.all_to_all(
        jnp.broadcast_to(value[None], (peers, *value.shape)), axis, 0, 0, tiled=True
    )


def shards(
    hidden_in,
    queries,
    lang_ids,
    owner_slot,
    enc_kv,
    attn_proj,
    norm_gain,
    router_proj,
    expert_ids,
    proj_in,
    proj_out,
):
    narrow_count = lax.axis_size("narrow")
    depth_count = lax.axis_size("depth")
    wide_count = lax.axis_size("wide")
    tok_rows, quarter = hidden_in.shape
    seg_rows, width = queries.shape
    experts = narrow_count
    peers = range(narrow_count)
    wide_at = lax.axis_index("wide")
    narrow_at = lax.axis_index("narrow")
    depth_at = lax.axis_index("depth")
    core, far = depth_at % 2, depth_at // 2
    core_perm = [(i, i ^ 1) for i in range(depth_count)]
    far_perm = [(i, i ^ 2) for i in range(depth_count)]

    def swap_perm(flip):
        return [
            (n * depth_count + d, d * narrow_count + (n ^ flip))
            for n in range(narrow_count)
            for d in range(depth_count)
        ]

    def around(values):
        return [values[0]] + [
            lax.ppermute(values[step], "narrow", ring(narrow_count, step)) for step in peers if step
        ]

    def to_core(value):
        return lax.ppermute(value, "depth", core_perm)

    def to_far(value):
        return lax.ppermute(value, "depth", far_perm)

    segment = to_all(queries, "wide")

    id_blocks = expert_ids.reshape(-1, tok_rows, 2)
    names = id_blocks[:, :, :, None] == jnp.arange(experts, dtype=jnp.int32)
    named = jnp.any(names, axis=2)
    ranks = jnp.where(named, jnp.cumsum(named.astype(jnp.int32), axis=1) - 1, -1)
    ranks = jnp.moveaxis(ranks, 2, 0)
    my_blocks = jnp.stack([core, 2 + core])
    around_to = (narrow_at + jnp.arange(narrow_count)) % narrow_count
    around_from = (narrow_at - jnp.arange(narrow_count)) % narrow_count
    send_slots = ranks[around_to][:, my_blocks].reshape(2 * narrow_count, tok_rows)
    get_slots = pick_at(ranks, narrow_at, 1)[around_from][:, :, None]
    my_ranks = pick_at(ranks, narrow_at)
    filled = my_ranks[:, None, :] == jnp.arange(CAP, dtype=jnp.int32)[None, :, None]
    here = jnp.arange(experts, dtype=jnp.int32) == narrow_at
    weigh = jnp.where(here[None, None, :], 1.0, -1.0) * named
    choose = jnp.sum(jnp.where(filled[:, :, :, None], weigh[:, None, :, :], 0.0), axis=2)
    choose = choose.reshape(-1, experts)
    choose = jnp.pad(jnp.concatenate([choose] * 3, axis=1), ((0, 0), (0, 128 - 3 * experts)))
    high = router_proj.astype(BF16)
    rest = router_proj - high.astype(F32)
    middle = rest.astype(BF16)
    low = (rest - middle.astype(F32)).astype(BF16)
    router = jnp.pad(
        jnp.concatenate([high, middle, low], axis=1), ((0, 0), (0, 128 - 3 * experts))
    )

    projs = around(
        [
            lax.dynamic_slice_in_dim(attn_proj, around_to[step] * quarter, quarter, 1)
            for step in peers
        ]
    )
    hidden_blocks = [
        lax.ppermute(hidden_in, ("narrow", "depth"), swap_perm(flip)) for flip in (0, 2)
    ]
    near_hidden = jnp.where(far == 0, hidden_blocks[0], hidden_blocks[1])
    far_hidden = jnp.where(far == 0, hidden_blocks[1], hidden_blocks[0])
    hidden_swapped = jnp.stack([near_hidden, far_hidden])
    router = router.reshape(narrow_count, quarter, 128)
    gain = norm_gain.reshape(narrow_count, 1, quarter)
    keys_t = enc_kv[0, 0].T
    values = enc_kv[0, 1]

    partial = attend(
        wide_at[None], owner_slot, lang_ids.reshape(wide_count, seg_rows), segment, keys_t, values
    )
    returned = lax.all_to_all(partial, "wide", split_axis=0, concat_axis=0, tiled=True)
    returned, projs, hidden_swapped, send_slots, get_slots, choose, router, gain = (
        lax.optimization_barrier(
            (returned, projs, hidden_swapped, send_slots, get_slots, choose, router, gain)
        )
    )
    context = jnp.sum(returned, axis=0, dtype=BF16)
    contexts = around([context] * narrow_count)

    send, keep = project(core[None], contexts, projs)
    near = (keep + to_core(send).astype(F32)).astype(BF16)
    w_in = hold(proj_in[0], send[0, :16, :128], 2)
    got, w_in = lax.optimization_barrier((to_far(near), w_in))
    residual, *boxes = dispatch(near, got, hidden_swapped, send_slots)
    own_rows = around(boxes)
    w_out = hold(proj_out[0], residual[0, :16, :128], 2)
    own_rows[1], w_out = lax.optimization_barrier((own_rows[1], w_out))
    other_rows = [to_core(part) for part in own_rows]
    own_resid = lax.ppermute(pick_at(residual, far), ("narrow", "depth"), swap_perm(0))

    out_send, out_keep = expert(
        jnp.stack([narrow_at, core]),
        own_rows,
        other_rows,
        gain,
        router,
        choose,
        w_in,
        w_out,
    )
    arrived = around(share(narrow_at[None], out_keep, to_core(out_send), narrow_count))
    far_send, own_sum = combine(far[None], get_slots, own_resid, arrived)
    return (own_sum + to_far(far_send).astype(F32)).astype(BF16)


def solution(mesh):
    return jax.shard_map(
        shards,
        mesh=mesh,
        in_specs=(
            P(("wide", "narrow"), "depth"),
            P("wide", ("narrow", "depth")),
            P(),
            P(),
            P("wide", None, None, ("narrow", "depth")),
            P(("narrow", "depth"), None),
            P(),
            P(),
            P("wide", None),
            P("narrow", None, "depth"),
            P("narrow", "depth", None),
        ),
        out_specs=P(("wide", "narrow"), "depth"),
        check_vma=False,
    )
```

```python
import jax
import jax.numpy as jnp
from jax import lax
from jax.experimental import pallas as pl
from jax.experimental.layout import Layout, with_layout_constraint
from jax.experimental.pallas import tpu as pltpu
from jax.sharding import PartitionSpec as P


HEAD_DIM = 64
CAP = 48
norm_eps = 1e-06
F32 = jnp.float32
BF16 = jnp.bfloat16
ROWS_BLOCK = 256


def dot(a, b):
    return jnp.dot(a, b, preferred_element_type=F32)


def iota(shape, dim):
    return lax.broadcasted_iota(jnp.int32, shape, dim)


def one_hot(flags):
    return jnp.where(flags, 1.0, 0.0).astype(BF16)


def attend_block(query, kv_ref):
    width = query.shape[1]
    head_of = iota((1, width), 1) // HEAD_DIM
    total = jnp.zeros(query.shape, F32)
    for head in range(width // HEAD_DIM):
        mine = head_of == head
        scores = lax.dot_general(
            jnp.where(mine, query, jnp.zeros_like(query)),
            kv_ref[0],
            (((1,), (1,)), ((), ())),
            preferred_element_type=F32,
        )
        weights = jnp.exp(scores - jnp.max(scores, axis=1, keepdims=True))
        norm = jnp.sum(weights, axis=1, keepdims=True)
        taken = dot(weights.astype(BF16), kv_ref[1])
        total = jnp.where(mine, taken / norm, total)
    return total


def attend_kernel(place, holder_ref, q_ref, kv_from, out_ref, kv_ref, attended, kv_sem):
    sources, rows, width = q_ref.shape
    wide_span = rows + 128
    kv_copy = pltpu.make_async_copy(kv_from, kv_ref, kv_sem)
    kv_copy.start()
    mine = holder_ref[...] == place[0]
    upto = one_hot(iota((rows, rows), 0) <= iota((rows, rows), 1))
    within = dot(one_hot(mine), upto)
    counts = within[:, rows - 1 :]
    begins = [jnp.int32(0)]
    before = jnp.zeros((sources, 1), F32)
    for source in range(sources):
        count = counts[source : source + 1, :]
        before = before + jnp.where(iota((sources, 1), 0) > source, count, 0.0)
        begins.append(begins[-1] + jnp.sum(count).astype(jnp.int32))
    pos = jnp.where(mine, within - 1.0 + before, -1.0)
    pos_row = pos.astype(jnp.int32)
    pos_col = pos.T.astype(jnp.int32)
    blocks = (begins[sources] + ROWS_BLOCK - 1) // ROWS_BLOCK
    rest = pl.ds(pl.multiple_of(blocks * ROWS_BLOCK, ROWS_BLOCK), wide_span)
    attended[rest, :] = jnp.zeros((wide_span, width), BF16)
    kv_copy.wait()

    def block(index, _):
        begin = pl.multiple_of(index * ROWS_BLOCK, ROWS_BLOCK)
        query = jnp.zeros((ROWS_BLOCK, width), F32)
        for source in range(sources):
            pick = one_hot(iota((ROWS_BLOCK, rows), 0) + begin == pos_row[source : source + 1, :])
            query = query + dot(pick, q_ref[source])
        total = attend_block((query * HEAD_DIM**-0.5).astype(BF16), kv_ref)
        attended[pl.ds(begin, ROWS_BLOCK), :] = total.astype(BF16)
        return 0

    lax.fori_loop(0, blocks, block, 0)
    for source in range(sources):
        at = pl.multiple_of((begins[source] // 16) * 16, 16)
        put = one_hot(iota((rows, wide_span), 1) + at == pos_col[:, source : source + 1])
        out_ref[source] = dot(put, attended[pl.ds(at, wide_span), :]).astype(BF16)


def attend(wide_at, holder, queries, keys_values):
    sources, rows, width = queries.shape
    capacity = sources * rows + rows + 128
    in_vmem = pl.BlockSpec(memory_space=pltpu.VMEM)
    return pl.pallas_call(
        attend_kernel,
        out_shape=jax.ShapeDtypeStruct(queries.shape, BF16),
        in_specs=[
            pl.BlockSpec(memory_space=pltpu.SMEM),
            in_vmem,
            in_vmem,
            pl.BlockSpec(memory_space=pl.ANY),
        ],
        out_specs=in_vmem,
        scratch_shapes=[
            pltpu.VMEM(keys_values.shape, BF16),
            pltpu.VMEM((capacity, width), BF16),
            pltpu.SemaphoreType.DMA,
        ],
        cost_estimate=pl.CostEstimate(flops=10**9, bytes_accessed=4 * 10**6, transcendentals=10**6),
        compiler_params=pltpu.CompilerParams(vmem_limit_bytes=32 * 1024 * 1024),
        name="attend",
    )(wide_at, holder, queries, keys_values)


ROUTE = 128


def route_kernel(place, slot_of, lang_ref, q_ref, box_ref, slot_ref, count_ref, fits_ref):
    sources, _, _ = box_ref.shape
    rows = q_ref.shape[0]
    langs = lang_ref[...]
    holder = jnp.zeros_like(langs)
    for lang in range(slot_of.shape[0]):
        holder = jnp.where(langs == lang, slot_of[lang], holder)
    pieces = langs.shape[0] // sources
    per_line = [
        jnp.sum(jnp.where(holder == which, 1.0, 0.0), axis=1, keepdims=True)
        for which in range(sources)
    ]
    per_line = jnp.concatenate(per_line, axis=1)
    join = one_hot(iota((sources, langs.shape[0]), 1) // pieces == iota((sources, langs.shape[0]), 0))
    counts = dot(join, per_line.astype(BF16))
    fits_ref[0] = (jnp.max(counts) <= ROUTE).astype(jnp.int32)
    here = jnp.sum(jnp.where(iota((1, sources), 1) == place[0], counts, 0.0), axis=1, keepdims=True)
    for source in range(sources):
        count_ref[source] = jnp.sum(here[source : source + 1, :]).astype(jnp.int32)
    line_of = iota(holder.shape, 0) - place[0] * pieces
    own = jnp.concatenate(
        [
            jnp.sum(jnp.where(line_of == piece, holder, 0), axis=0, keepdims=True)
            for piece in range(pieces)
        ],
        axis=1,
    )
    goes = own == iota((sources, rows), 0)
    upto = one_hot(iota((rows, rows), 0) <= iota((rows, rows), 1))
    slots = jnp.where(goes, dot(one_hot(goes), upto) - 1.0, -1.0).astype(jnp.int32)
    slot_ref[...] = slots
    for which in range(sources):
        pick = one_hot(iota((ROUTE, rows), 0) == slots[which : which + 1, :])
        box_ref[which] = dot(pick, q_ref[...]).astype(BF16)


def route(wide_at, owner_slot, lang_ids, queries, sources):
    rows, width = queries.shape
    in_vmem = pl.BlockSpec(memory_space=pltpu.VMEM)
    in_smem = pl.BlockSpec(memory_space=pltpu.SMEM)
    return pl.pallas_call(
        route_kernel,
        out_shape=(
            jax.ShapeDtypeStruct((sources, ROUTE, width), BF16),
            jax.ShapeDtypeStruct((sources, rows), jnp.int32),
            jax.ShapeDtypeStruct((sources,), jnp.int32),
            jax.ShapeDtypeStruct((1,), jnp.int32),
        ),
        in_specs=[in_smem, in_smem, in_vmem, in_vmem],
        out_specs=(in_vmem, in_vmem, in_smem, in_smem),
        cost_estimate=pl.CostEstimate(flops=10**8, bytes_accessed=10**6, transcendentals=0),
        compiler_params=pltpu.CompilerParams(vmem_limit_bytes=16 * 1024 * 1024),
        name="route",
    )(wide_at, owner_slot, lang_ids.reshape(-1, 128), queries)


def routed_kernel(counts, q_ref, kv_from, out_ref, kv_ref, attended, kv_sem):
    sources, span, width = q_ref.shape
    kv_copy = pltpu.make_async_copy(kv_from, kv_ref, kv_sem)
    kv_copy.start()
    begins = [0]
    for source in range(sources):
        begins.append(begins[-1] + counts[source])
    blocks = (begins[sources] + ROWS_BLOCK - 1) // ROWS_BLOCK
    rest = pl.ds(pl.multiple_of(blocks * ROWS_BLOCK, ROWS_BLOCK), 2 * span)
    attended[rest, :] = jnp.zeros((2 * span, width), BF16)
    lane = iota((1, 2 * span), 1)
    ranks = []
    for source in range(0, sources, 2):
        first = jnp.where(lane < counts[source], begins[source] + lane, -1)
        second = jnp.where(lane - span < counts[source + 1], begins[source + 1] + lane - span, -1)
        ranks.append(jnp.where(lane < span, first, second))
    kv_copy.wait()

    def block(index, _):
        begin = pl.multiple_of(index * ROWS_BLOCK, ROWS_BLOCK)
        query = jnp.zeros((ROWS_BLOCK, width), F32)
        for pair, rank in enumerate(ranks):
            pick = one_hot(iota((ROWS_BLOCK, 2 * span), 0) + begin == rank)
            query = query + dot(pick, q_ref[2 * pair : 2 * pair + 2].reshape(2 * span, width))
        total = attend_block((query * HEAD_DIM**-0.5).astype(BF16), kv_ref)
        attended[pl.ds(begin, ROWS_BLOCK), :] = total.astype(BF16)
        return 0

    lax.fori_loop(0, blocks, block, 0)
    for source in range(sources):
        at = pl.multiple_of((begins[source] // 16) * 16, 16)
        shift = begins[source] - at
        put = one_hot(iota((span, 2 * span), 1) == iota((span, 2 * span), 0) + shift)
        out_ref[source] = dot(put, attended[pl.ds(at, 2 * span), :]).astype(BF16)


def attend_routed(counts, queries, keys_values):
    sources, span, width = queries.shape
    capacity = sources * span + 2 * ROWS_BLOCK
    in_vmem = pl.BlockSpec(memory_space=pltpu.VMEM)
    return pl.pallas_call(
        routed_kernel,
        out_shape=jax.ShapeDtypeStruct(queries.shape, BF16),
        in_specs=[
            pl.BlockSpec(memory_space=pltpu.SMEM),
            in_vmem,
            pl.BlockSpec(memory_space=pl.ANY),
        ],
        out_specs=in_vmem,
        scratch_shapes=[
            pltpu.VMEM(keys_values.shape, BF16),
            pltpu.VMEM((capacity, width), BF16),
            pltpu.SemaphoreType.DMA,
        ],
        cost_estimate=pl.CostEstimate(flops=10**9, bytes_accessed=4 * 10**6, transcendentals=10**6),
        compiler_params=pltpu.CompilerParams(vmem_limit_bytes=32 * 1024 * 1024),
        name="attend",
    )(counts, queries, keys_values)


def gather_kernel(slot_ref, box_ref, out_ref):
    sources, span, width = box_ref.shape
    rows = out_ref.shape[0]
    slot_col = slot_ref[...].astype(F32).T.astype(jnp.int32)
    total = jnp.zeros((rows, width), F32)
    for which in range(sources):
        pick = one_hot(iota((rows, span), 1) == slot_col[:, which : which + 1])
        total = total + dot(pick, box_ref[which])
    out_ref[...] = total.astype(BF16)


def gather_rows(slots, boxes):
    in_vmem = pl.BlockSpec(memory_space=pltpu.VMEM)
    return pl.pallas_call(
        gather_kernel,
        out_shape=jax.ShapeDtypeStruct((slots.shape[1], boxes.shape[2]), BF16),
        in_specs=[in_vmem, in_vmem],
        out_specs=in_vmem,
        cost_estimate=pl.CostEstimate(flops=10**8, bytes_accessed=10**6, transcendentals=0),
        compiler_params=pltpu.CompilerParams(vmem_limit_bytes=16 * 1024 * 1024),
        name="gather",
    )(slots, boxes)


def project_kernel(place, *refs):
    parts = (len(refs) - 3) // 2
    ctx_refs, proj_refs = refs[:parts], refs[parts : 2 * parts]
    send_ref, keep_ref, full = refs[2 * parts :]
    rows = send_ref.shape[1]
    acc = dot(ctx_refs[0][...], proj_refs[0][...])
    for part in range(1, parts):
        acc = acc + dot(ctx_refs[part][...], proj_refs[part][...])
    full[...] = acc
    core = place[0]
    for far in range(2):
        gone = pl.multiple_of((far * 2 + 1 - core) * rows, rows)
        kept = pl.multiple_of((far * 2 + core) * rows, rows)
        send_ref[far] = full[pl.ds(gone, rows), :].astype(BF16)
        keep_ref[far] = full[pl.ds(kept, rows), :]


def project(core, contexts, projs):
    rows, _ = contexts[0].shape
    cols = projs[0].shape[1]
    in_vmem = pl.BlockSpec(memory_space=pltpu.VMEM)
    return pl.pallas_call(
        project_kernel,
        out_shape=(
            jax.ShapeDtypeStruct((2, rows // 4, cols), BF16),
            jax.ShapeDtypeStruct((2, rows // 4, cols), F32),
        ),
        in_specs=[pl.BlockSpec(memory_space=pltpu.SMEM)] + [in_vmem] * (len(contexts) + len(projs)),
        out_specs=(in_vmem, in_vmem),
        scratch_shapes=[pltpu.VMEM((rows, cols), F32)],
        cost_estimate=pl.CostEstimate(flops=10**9, bytes_accessed=4 * 10**6, transcendentals=0),
        compiler_params=pltpu.CompilerParams(vmem_limit_bytes=24 * 1024 * 1024),
        name="project",
    )(core, *contexts, *projs)


def dispatch_kernel(place, near_ref, got_ref, hidden_ref, slot_ref, own_ref, *refs):
    box_refs, resid_ref = refs[:-1], refs[-1]
    for far in range(2):
        summed = near_ref[far].astype(F32) + got_ref[far].astype(F32)
        residual = (hidden_ref[far].astype(F32) + summed).astype(BF16)
        resid_ref[far] = residual
        for step, box_ref in enumerate(box_refs):
            index = step * 2 + far
            pick = one_hot(iota((CAP, residual.shape[0]), 0) == slot_ref[index : index + 1, :])
            box_ref[far] = dot(pick, residual).astype(BF16)
    own_ref[...] = resid_ref[place[0]]


def dispatch(far, near, got, hidden, slots):
    _, _, cols = near.shape
    steps = slots.shape[0] // 2
    in_vmem = pl.BlockSpec(memory_space=pltpu.VMEM)
    return pl.pallas_call(
        dispatch_kernel,
        out_shape=(jax.ShapeDtypeStruct(near.shape[1:], BF16),)
        + (jax.ShapeDtypeStruct((2, CAP, cols), BF16),) * steps,
        in_specs=[pl.BlockSpec(memory_space=pltpu.SMEM)] + [in_vmem] * 4,
        out_specs=(in_vmem,) * (1 + steps),
        scratch_shapes=[pltpu.VMEM(near.shape, BF16)],
        cost_estimate=pl.CostEstimate(flops=10**8, bytes_accessed=2 * 10**6, transcendentals=0),
        compiler_params=pltpu.CompilerParams(vmem_limit_bytes=8 * 1024 * 1024),
        name="dispatch",
    )(far, near, got, hidden, slots)


def hold_kernel(from_ref, _, held_ref, sems):
    pieces = sems.shape[0]
    rows = from_ref.shape[0] // pieces
    copies = [
        pltpu.make_async_copy(
            from_ref.at[pl.ds(piece * rows, rows)], held_ref.at[pl.ds(piece * rows, rows)], sems.at[piece]
        )
        for piece in range(pieces)
    ]
    for copy in copies:
        copy.start()
    for copy in copies:
        copy.wait()


def hold(weight, after, grant):
    in_vmem = pl.BlockSpec(memory_space=pltpu.VMEM)
    return pl.pallas_call(
        hold_kernel,
        out_shape=jax.ShapeDtypeStruct(weight.shape, weight.dtype),
        in_specs=[pl.BlockSpec(memory_space=pltpu.HBM), pl.BlockSpec(memory_space=pl.ANY)],
        out_specs=in_vmem,
        scratch_shapes=[pltpu.SemaphoreType.DMA((8,))],
        cost_estimate=pl.CostEstimate(flops=4 * 10**9, bytes_accessed=10**7, transcendentals=0),
        compiler_params=pltpu.CompilerParams(vmem_limit_bytes=grant * 1024 * 1024),
        name="hold",
    )(weight, after)


IN_COLS = 640
OUT_COLS = 1024


def expert_kernel(place, *refs):
    parts = 4
    row_refs = refs[: 2 * parts]
    gain_ref, router_ref, choose_ref, w_in, w_out, send_ref, keep_ref = refs[2 * parts : 2 * parts + 7]
    rows_all, hidden = refs[2 * parts + 7 :]
    narrow_at, core = place[0], place[1]
    features, hidden_units = w_in.shape
    _, slots, quarter = row_refs[0].shape
    blocks = [lax.rem(narrow_at + parts - step, parts) for step in range(parts)]

    for which, side in ((0, core), (1, 1 - core)):
        for far in range(2):
            squares = jnp.zeros((slots, 1), F32)
            for part in range(parts):
                rows = row_refs[which * parts + part][far].astype(F32)
                squares = squares + jnp.sum(rows * rows, axis=1, keepdims=True)
            inverse = lax.rsqrt(squares / features + norm_eps)
            at = pl.multiple_of((far * 2 + side) * slots, 16)
            for part in range(parts):
                rows = row_refs[which * parts + part][far].astype(F32)
                normed = rows * inverse * gain_ref[blocks[part]]
                rows_all[part, pl.ds(at, slots), :] = normed.astype(BF16)
    logits = jnp.zeros((4 * slots, 3 * router_ref.shape[0]), F32)
    for part in range(parts):
        exact = router_ref[:, pl.ds(pl.multiple_of(blocks[part] * quarter, quarter), quarter)]
        high = exact.astype(BF16)
        rest = exact - high.astype(F32)
        middle = rest.astype(BF16)
        low = (rest - middle.astype(F32)).astype(BF16)
        pieces = jnp.concatenate([high.astype(F32), middle.astype(F32), low.astype(F32)], axis=0)
        logits = logits + lax.dot_general(
            rows_all[part],
            pieces.astype(BF16),
            (((1,), (1,)), ((), ())),
            preferred_element_type=F32,
        )
    differ = jnp.sum(logits * choose_ref[:, : logits.shape[1]], axis=1, keepdims=True)
    gate = 1.0 / (1.0 + jnp.exp(-differ))
    for step in range(hidden_units // IN_COLS):
        cols = slice(step * IN_COLS, (step + 1) * IN_COLS)
        acc = None
        for part in range(parts):
            at = pl.multiple_of(blocks[part] * quarter, quarter)
            term = dot(rows_all[part], w_in[pl.ds(at, quarter), cols])
            acc = term if acc is None else acc + term
        hidden[:, cols] = jax.nn.gelu(acc, approximate=True).astype(BF16)
    for kept in range(2):
        side = core if kept else 1 - core
        for far in range(2):
            for step in range(quarter // OUT_COLS):
                at = pl.multiple_of((far * 2 + side) * quarter + step * OUT_COLS, OUT_COLS)
                acc = dot(hidden[...], w_out[:, pl.ds(at, OUT_COLS)]) * gate
                cols = slice(step * OUT_COLS, (step + 1) * OUT_COLS)
                if kept:
                    keep_ref[far, :, cols] = acc
                else:
                    send_ref[far, :, cols] = acc.astype(BF16)


def expert(place, own, other, gain, router, choose, w_in, w_out):
    _, slots, quarter = own[0].shape
    parts = len(own)
    rows = 4 * slots
    _, units = w_in.shape
    in_vmem = pl.BlockSpec(memory_space=pltpu.VMEM)
    return pl.pallas_call(
        expert_kernel,
        out_shape=(
            jax.ShapeDtypeStruct((2, rows, quarter), BF16),
            jax.ShapeDtypeStruct((2, rows, quarter), F32),
        ),
        in_specs=[pl.BlockSpec(memory_space=pltpu.SMEM)]
        + [in_vmem] * (2 * parts + 5),
        out_specs=(in_vmem, in_vmem),
        scratch_shapes=[
            pltpu.VMEM((parts, rows, quarter), BF16),
            pltpu.VMEM((rows, units), BF16),
        ],
        cost_estimate=pl.CostEstimate(flops=4 * 10**9, bytes_accessed=24 * 10**6, transcendentals=10**5),
        compiler_params=pltpu.CompilerParams(vmem_limit_bytes=12 * 1024 * 1024),
        name="expert",
    )(place, *own, *other, gain, router, choose, w_in, w_out)


def share_kernel(place, keep_ref, got_ref, *box_refs):
    slots = box_refs[0].shape[1]
    for step, box_ref in enumerate(box_refs):
        block = lax.rem(place[0] + step, len(box_refs))
        at = pl.ds(pl.multiple_of(block * slots, 16), slots)
        for far in range(2):
            box_ref[far] = (keep_ref[far, at, :] + got_ref[far, at, :].astype(F32)).astype(BF16)


def share(place, keep, got, peers):
    _, rows, cols = keep.shape
    in_vmem = pl.BlockSpec(memory_space=pltpu.VMEM)
    return pl.pallas_call(
        share_kernel,
        out_shape=(jax.ShapeDtypeStruct((2, rows // peers, cols), BF16),) * peers,
        in_specs=[pl.BlockSpec(memory_space=pltpu.SMEM), in_vmem, in_vmem],
        out_specs=(in_vmem,) * peers,
        cost_estimate=pl.CostEstimate(flops=10**7, bytes_accessed=4 * 10**6, transcendentals=0),
        compiler_params=pltpu.CompilerParams(vmem_limit_bytes=8 * 1024 * 1024),
        name="share",
    )(place, keep, got)


def combine_kernel(place, slot_ref, resid_ref, *refs):
    box_refs, (send_ref, keep_ref, both) = refs[:-3], refs[-3:]
    tokens = slot_ref.shape[1]
    for far in range(2):
        acc = jnp.zeros(both.shape[1:], F32)
        for step, box_ref in enumerate(box_refs):
            pick = one_hot(iota((CAP, tokens), 0) == slot_ref[step : step + 1, :])
            acc = acc + lax.dot_general(
                pick, box_ref[far], (((0,), (0,)), ((), ())), preferred_element_type=F32
            )
        both[far] = acc
    send_ref[...] = both[1 - place[0]].astype(BF16)
    keep_ref[...] = both[place[0]] + resid_ref[...].astype(F32)


def combine(place, slots, resid, boxes):
    in_vmem = pl.BlockSpec(memory_space=pltpu.VMEM)
    return pl.pallas_call(
        combine_kernel,
        out_shape=(
            jax.ShapeDtypeStruct(resid.shape, BF16),
            jax.ShapeDtypeStruct(resid.shape, F32),
        ),
        in_specs=[pl.BlockSpec(memory_space=pltpu.SMEM)] + [in_vmem] * (2 + len(boxes)),
        out_specs=(in_vmem, in_vmem),
        scratch_shapes=[pltpu.VMEM((2, *resid.shape), F32)],
        cost_estimate=pl.CostEstimate(flops=10**8, bytes_accessed=2 * 10**6, transcendentals=0),
        compiler_params=pltpu.CompilerParams(vmem_limit_bytes=8 * 1024 * 1024),
        name="combine",
    )(place, slots, resid, *boxes)


def ring(count, step):
    return [(i, (i + step) % count) for i in range(count)]


def pick_at(values, index, axis=0):
    return lax.dynamic_index_in_dim(values, index, axis, keepdims=False)


def body(
    hidden_in,
    queries,
    lang_ids,
    owner_slot,
    enc_kv,
    attn_proj,
    norm_gain,
    router_proj,
    expert_ids,
    proj_in,
    proj_out,
):
    narrow_count = lax.axis_size("narrow")
    depth_count = lax.axis_size("depth")
    wide_count = lax.axis_size("wide")
    tok_rows, quarter = hidden_in.shape
    seg_rows, _ = queries.shape
    experts = narrow_count
    peers = range(narrow_count)
    wide_at = lax.axis_index("wide")
    narrow_at = lax.axis_index("narrow")
    depth_at = lax.axis_index("depth")
    core, far = depth_at % 2, depth_at // 2
    core_perm = [(i, i ^ 1) for i in range(depth_count)]
    far_perm = [(i, i ^ 2) for i in range(depth_count)]

    def swap_perm(flip):
        return [
            (n * depth_count + d, d * narrow_count + (n ^ flip))
            for n in range(narrow_count)
            for d in range(depth_count)
        ]

    def around(values):
        return [values[0]] + [
            lax.ppermute(values[step], "narrow", ring(narrow_count, step))
            for step in peers
            if step
        ]

    def to_core(value):
        return lax.ppermute(value, "depth", core_perm)

    def to_far(value):
        return lax.ppermute(value, "depth", far_perm)

    around_to = (narrow_at + jnp.arange(narrow_count)) % narrow_count

    def prepared(hidden_in, expert_ids):
        id_blocks = expert_ids.reshape(-1, tok_rows, 2)
        names = id_blocks[:, :, :, None] == jnp.arange(experts, dtype=jnp.int32)
        named = jnp.any(names, axis=2)
        ranks = jnp.where(named, jnp.cumsum(named.astype(jnp.int32), axis=1) - 1, -1)
        ranks = jnp.moveaxis(ranks, 2, 0)
        my_blocks = jnp.stack([core, 2 + core])
        around_from = (narrow_at - jnp.arange(narrow_count)) % narrow_count
        send_slots = ranks[around_to][:, my_blocks].reshape(2 * narrow_count, tok_rows)
        get_slots = pick_at(ranks, narrow_at, 1)[around_from]
        my_ranks = pick_at(ranks, narrow_at)
        filled = my_ranks[:, None, :] == jnp.arange(CAP, dtype=jnp.int32)[None, :, None]
        here = jnp.arange(experts, dtype=jnp.int32) == narrow_at
        weigh = jnp.where(here[None, None, :], 1.0, -1.0) * named
        choose = jnp.sum(jnp.where(filled[:, :, :, None], weigh[:, None, :, :], 0.0), axis=2)
        choose = choose.reshape(-1, experts)
        choose = jnp.pad(jnp.concatenate([choose] * 3, axis=1), ((0, 0), (0, 128 - 3 * experts)))
        hidden_blocks = [
            lax.ppermute(hidden_in, ("narrow", "depth"), swap_perm(flip)) for flip in (0, 2)
        ]
        near_hidden = jnp.where(far == 0, hidden_blocks[0], hidden_blocks[1])
        far_hidden = jnp.where(far == 0, hidden_blocks[1], hidden_blocks[0])
        hidden_swapped = jnp.stack([near_hidden, far_hidden])
        return tuple(
            with_layout_constraint(value, Layout(tuple(range(value.ndim))))
            for value in (hidden_swapped, send_slots, get_slots, choose)
        )

    def spread():
        projs = around(
            [
                lax.dynamic_slice_in_dim(attn_proj, around_to[step] * quarter, quarter, 1)
                for step in peers
            ],
        )
        return tuple(projs)

    def exchanged(boxes, attend_to, gathered):
        segment = lax.all_to_all(boxes, "wide", split_axis=0, concat_axis=0, tiled=True)
        projs = spread()
        partial, *late = lax.optimization_barrier(
            (attend_to(segment), hidden_in, expert_ids)
        )
        returned = lax.all_to_all(partial, "wide", split_axis=0, concat_axis=0, tiled=True)
        returned, projs, ready = lax.optimization_barrier((returned, projs, prepared(*late)))
        return gathered(returned), projs, ready

    def routed(boxes):
        return exchanged(
            boxes,
            lambda segment: attend_routed(counts, segment, enc_kv[0]),
            lambda returned: gather_rows(slots, returned),
        )

    def general(_):
        langs = lang_ids.reshape(wide_count, seg_rows)
        match = langs[:, :, None] == jnp.arange(owner_slot.shape[0], dtype=jnp.int32)
        holder = jnp.sum(jnp.where(match, owner_slot, 0), axis=2)
        return exchanged(
            jnp.broadcast_to(queries[None], (wide_count, *queries.shape)),
            lambda segment: attend(wide_at[None], holder, segment, enc_kv[0]),
            lambda returned: jnp.sum(returned, axis=0, dtype=BF16),
        )

    boxes, slots, counts, fits = route(wide_at[None], owner_slot, lang_ids, queries, wide_count)
    context, projs, ready = lax.cond(fits[0] == 1, routed, general, boxes)
    hidden_swapped, send_slots, get_slots, choose = ready
    contexts = around([context] * narrow_count)

    send, keep = project(core[None], contexts, projs)
    near = (keep + to_core(send).astype(F32)).astype(BF16)
    w_in = hold(proj_in[0], send, 2)
    got, w_in = lax.optimization_barrier((to_far(near), w_in))
    residual, *boxes = dispatch(far[None], near, got, hidden_swapped, send_slots)
    own_rows = around(boxes)
    w_out = hold(proj_out[0], residual, 2)
    own_resid = lax.ppermute(residual, ("narrow", "depth"), swap_perm(0))
    own_rows[1], w_out, own_resid = lax.optimization_barrier((own_rows[1], w_out, own_resid))
    other_rows = [to_core(part) for part in own_rows]

    out_send, out_keep = expert(
        jnp.stack([narrow_at, core]),
        own_rows,
        other_rows,
        norm_gain.reshape(narrow_count, 1, quarter),
        router_proj.T,
        choose,
        w_in,
        w_out,
    )
    arrived = around(share(narrow_at[None], out_keep, to_core(out_send), narrow_count))
    far_send, own_sum = combine(far[None], get_slots, own_resid, arrived)
    return (own_sum + to_far(far_send).astype(F32)).astype(BF16)


def solution(mesh):
    return jax.shard_map(
        body,
        mesh=mesh,
        in_specs=(
            P(("wide", "narrow"), "depth"),
            P("wide", ("narrow", "depth")),
            P(),
            P(),
            P("wide", None, None, ("narrow", "depth")),
            P(("narrow", "depth"), None),
            P(),
            P(),
            P("wide", None),
            P("narrow", None, "depth"),
            P("narrow", "depth", None),
        ),
        out_specs=P(("wide", "narrow"), "depth"),
        check_vma=False,
    )
```

```python
import jax
import jax.numpy as jnp
from jax import lax
from jax.experimental import pallas as pl
from jax.experimental.layout import Layout, with_layout_constraint
from jax.experimental.pallas import tpu as pltpu
from jax.sharding import PartitionSpec as P


HEAD_DIM = 64
CAP = 48
norm_eps = 1e-06
F32 = jnp.float32
BF16 = jnp.bfloat16
ROWS_BLOCK = 256


def dot(a, b):
    return jnp.dot(a, b, preferred_element_type=F32)


def iota(shape, dim):
    return lax.broadcasted_iota(jnp.int32, shape, dim)


def one_hot(flags):
    return jnp.where(flags, 1.0, 0.0).astype(BF16)


def attend_block(query, kv_ref):
    width = query.shape[1]
    head_of = iota((1, width), 1) // HEAD_DIM
    total = jnp.zeros(query.shape, F32)
    for head in range(width // HEAD_DIM):
        mine = head_of == head
        scores = lax.dot_general(
            jnp.where(mine, query, jnp.zeros_like(query)),
            kv_ref[0],
            (((1,), (1,)), ((), ())),
            preferred_element_type=F32,
        )
        weights = jnp.exp(scores - jnp.max(scores, axis=1, keepdims=True))
        norm = jnp.sum(weights, axis=1, keepdims=True)
        taken = dot(weights.astype(BF16), kv_ref[1])
        total = jnp.where(mine, taken / norm, total)
    return total


def attend_kernel(place, holder_ref, q_ref, kv_from, out_ref, kv_ref, attended, kv_sem):
    sources, rows, width = q_ref.shape
    wide_span = rows + 128
    kv_copy = pltpu.make_async_copy(kv_from, kv_ref, kv_sem)
    kv_copy.start()
    mine = holder_ref[...] == place[0]
    upto = one_hot(iota((rows, rows), 0) <= iota((rows, rows), 1))
    within = dot(one_hot(mine), upto)
    counts = within[:, rows - 1 :]
    begins = [jnp.int32(0)]
    before = jnp.zeros((sources, 1), F32)
    for source in range(sources):
        count = counts[source : source + 1, :]
        before = before + jnp.where(iota((sources, 1), 0) > source, count, 0.0)
        begins.append(begins[-1] + jnp.sum(count).astype(jnp.int32))
    pos = jnp.where(mine, within - 1.0 + before, -1.0)
    pos_row = pos.astype(jnp.int32)
    pos_col = pos.T.astype(jnp.int32)
    blocks = (begins[sources] + ROWS_BLOCK - 1) // ROWS_BLOCK
    rest = pl.ds(pl.multiple_of(blocks * ROWS_BLOCK, ROWS_BLOCK), wide_span)
    attended[rest, :] = jnp.zeros((wide_span, width), BF16)
    kv_copy.wait()

    def block(index, _):
        begin = pl.multiple_of(index * ROWS_BLOCK, ROWS_BLOCK)
        query = jnp.zeros((ROWS_BLOCK, width), F32)
        for source in range(sources):
            pick = one_hot(iota((ROWS_BLOCK, rows), 0) + begin == pos_row[source : source + 1, :])
            query = query + dot(pick, q_ref[source])
        total = attend_block((query * HEAD_DIM**-0.5).astype(BF16), kv_ref)
        attended[pl.ds(begin, ROWS_BLOCK), :] = total.astype(BF16)
        return 0

    lax.fori_loop(0, blocks, block, 0)
    for source in range(sources):
        at = pl.multiple_of((begins[source] // 16) * 16, 16)
        put = one_hot(iota((rows, wide_span), 1) + at == pos_col[:, source : source + 1])
        out_ref[source] = dot(put, attended[pl.ds(at, wide_span), :]).astype(BF16)


def attend(wide_at, holder, queries, keys_values):
    sources, rows, width = queries.shape
    capacity = sources * rows + rows + 128
    in_vmem = pl.BlockSpec(memory_space=pltpu.VMEM)
    return pl.pallas_call(
        attend_kernel,
        out_shape=jax.ShapeDtypeStruct(queries.shape, BF16),
        in_specs=[
            pl.BlockSpec(memory_space=pltpu.SMEM),
            in_vmem,
            in_vmem,
            pl.BlockSpec(memory_space=pl.ANY),
        ],
        out_specs=in_vmem,
        scratch_shapes=[
            pltpu.VMEM(keys_values.shape, BF16),
            pltpu.VMEM((capacity, width), BF16),
            pltpu.SemaphoreType.DMA,
        ],
        cost_estimate=pl.CostEstimate(flops=10**9, bytes_accessed=4 * 10**6, transcendentals=10**6),
        compiler_params=pltpu.CompilerParams(vmem_limit_bytes=32 * 1024 * 1024),
        name="attend",
    )(wide_at, holder, queries, keys_values)


ROUTE = 128


def route_kernel(place, slot_of, lang_ref, q_ref, box_ref, slot_ref, count_ref, fits_ref):
    sources, _, _ = box_ref.shape
    rows = q_ref.shape[0]
    langs = lang_ref[...]
    holder = jnp.zeros_like(langs)
    for lang in range(slot_of.shape[0]):
        holder = jnp.where(langs == lang, slot_of[lang], holder)
    pieces = langs.shape[0] // sources
    per_line = [
        jnp.sum(jnp.where(holder == which, 1.0, 0.0), axis=1, keepdims=True)
        for which in range(sources)
    ]
    per_line = jnp.concatenate(per_line, axis=1)
    join = one_hot(iota((sources, langs.shape[0]), 1) // pieces == iota((sources, langs.shape[0]), 0))
    counts = dot(join, per_line.astype(BF16))
    fits_ref[0] = (jnp.max(counts) <= ROUTE).astype(jnp.int32)
    here = jnp.sum(jnp.where(iota((1, sources), 1) == place[0], counts, 0.0), axis=1, keepdims=True)
    for source in range(sources):
        count_ref[source] = jnp.sum(here[source : source + 1, :]).astype(jnp.int32)
    line_of = iota(holder.shape, 0) - place[0] * pieces
    own = jnp.concatenate(
        [
            jnp.sum(jnp.where(line_of == piece, holder, 0), axis=0, keepdims=True)
            for piece in range(pieces)
        ],
        axis=1,
    )
    goes = own == iota((sources, rows), 0)
    upto = one_hot(iota((rows, rows), 0) <= iota((rows, rows), 1))
    slots = jnp.where(goes, dot(one_hot(goes), upto) - 1.0, -1.0).astype(jnp.int32)
    slot_ref[...] = slots
    for which in range(sources):
        pick = one_hot(iota((ROUTE, rows), 0) == slots[which : which + 1, :])
        box_ref[which] = dot(pick, q_ref[...]).astype(BF16)


def route(wide_at, owner_slot, lang_ids, queries, sources):
    rows, width = queries.shape
    in_vmem = pl.BlockSpec(memory_space=pltpu.VMEM)
    in_smem = pl.BlockSpec(memory_space=pltpu.SMEM)
    return pl.pallas_call(
        route_kernel,
        out_shape=(
            jax.ShapeDtypeStruct((sources, ROUTE, width), BF16),
            jax.ShapeDtypeStruct((sources, rows), jnp.int32),
            jax.ShapeDtypeStruct((sources,), jnp.int32),
            jax.ShapeDtypeStruct((1,), jnp.int32),
        ),
        in_specs=[in_smem, in_smem, in_vmem, in_vmem],
        out_specs=(in_vmem, in_vmem, in_smem, in_smem),
        cost_estimate=pl.CostEstimate(flops=10**8, bytes_accessed=10**6, transcendentals=0),
        compiler_params=pltpu.CompilerParams(vmem_limit_bytes=16 * 1024 * 1024),
        name="route",
    )(wide_at, owner_slot, lang_ids.reshape(-1, 128), queries)


def routed_kernel(counts, q_ref, kv_from, out_ref, kv_ref, attended, kv_sem):
    sources, span, width = q_ref.shape
    kv_copy = pltpu.make_async_copy(kv_from, kv_ref, kv_sem)
    kv_copy.start()
    begins = [0]
    for source in range(sources):
        begins.append(begins[-1] + counts[source])
    blocks = (begins[sources] + ROWS_BLOCK - 1) // ROWS_BLOCK
    rest = pl.ds(pl.multiple_of(blocks * ROWS_BLOCK, ROWS_BLOCK), 2 * span)
    attended[rest, :] = jnp.zeros((2 * span, width), BF16)
    lane = iota((1, 2 * span), 1)
    ranks = []
    for source in range(0, sources, 2):
        first = jnp.where(lane < counts[source], begins[source] + lane, -1)
        second = jnp.where(lane - span < counts[source + 1], begins[source + 1] + lane - span, -1)
        ranks.append(jnp.where(lane < span, first, second))
    kv_copy.wait()

    def block(index, _):
        begin = pl.multiple_of(index * ROWS_BLOCK, ROWS_BLOCK)
        query = jnp.zeros((ROWS_BLOCK, width), F32)
        for pair, rank in enumerate(ranks):
            pick = one_hot(iota((ROWS_BLOCK, 2 * span), 0) + begin == rank)
            query = query + dot(pick, q_ref[2 * pair : 2 * pair + 2].reshape(2 * span, width))
        total = attend_block((query * HEAD_DIM**-0.5).astype(BF16), kv_ref)
        attended[pl.ds(begin, ROWS_BLOCK), :] = total.astype(BF16)
        return 0

    lax.fori_loop(0, blocks, block, 0)
    for source in range(sources):
        at = pl.multiple_of((begins[source] // 16) * 16, 16)
        shift = begins[source] - at
        put = one_hot(iota((span, 2 * span), 1) == iota((span, 2 * span), 0) + shift)
        out_ref[source] = dot(put, attended[pl.ds(at, 2 * span), :]).astype(BF16)


def attend_routed(counts, queries, keys_values):
    sources, span, width = queries.shape
    capacity = sources * span + 2 * ROWS_BLOCK
    in_vmem = pl.BlockSpec(memory_space=pltpu.VMEM)
    return pl.pallas_call(
        routed_kernel,
        out_shape=jax.ShapeDtypeStruct(queries.shape, BF16),
        in_specs=[
            pl.BlockSpec(memory_space=pltpu.SMEM),
            in_vmem,
            pl.BlockSpec(memory_space=pl.ANY),
        ],
        out_specs=in_vmem,
        scratch_shapes=[
            pltpu.VMEM(keys_values.shape, BF16),
            pltpu.VMEM((capacity, width), BF16),
            pltpu.SemaphoreType.DMA,
        ],
        cost_estimate=pl.CostEstimate(flops=10**9, bytes_accessed=4 * 10**6, transcendentals=10**6),
        compiler_params=pltpu.CompilerParams(vmem_limit_bytes=32 * 1024 * 1024),
        name="attend",
    )(counts, queries, keys_values)


def gather_kernel(slot_ref, box_ref, out_ref):
    sources, span, width = box_ref.shape
    rows = out_ref.shape[0]
    slot_col = slot_ref[...].astype(F32).T.astype(jnp.int32)
    total = jnp.zeros((rows, width), F32)
    for which in range(sources):
        pick = one_hot(iota((rows, span), 1) == slot_col[:, which : which + 1])
        total = total + dot(pick, box_ref[which])
    out_ref[...] = total.astype(BF16)


def gather_rows(slots, boxes):
    in_vmem = pl.BlockSpec(memory_space=pltpu.VMEM)
    return pl.pallas_call(
        gather_kernel,
        out_shape=jax.ShapeDtypeStruct((slots.shape[1], boxes.shape[2]), BF16),
        in_specs=[in_vmem, in_vmem],
        out_specs=in_vmem,
        cost_estimate=pl.CostEstimate(flops=10**8, bytes_accessed=10**6, transcendentals=0),
        compiler_params=pltpu.CompilerParams(vmem_limit_bytes=16 * 1024 * 1024),
        name="gather",
    )(slots, boxes)


def begin_kernel(*refs):
    parts = (len(refs) - 2) // 4
    late_from, late_to, sems = refs[2 * parts : 3 * parts], refs[3 * parts + 1 : 4 * parts + 1], refs[-1]
    copies = [
        pltpu.make_async_copy(late_from[part], late_to[part], sems.at[part]) for part in range(parts)
    ]
    for copy in copies:
        copy.start()
    acc = dot(refs[0][...], refs[parts][...])
    for part in range(1, parts):
        acc = acc + dot(refs[part][...], refs[parts + part][...])
    refs[3 * parts][...] = acc
    for copy in copies:
        copy.wait()


def project_kernel(place, begun_ref, *refs):
    parts = (len(refs) - 3) // 2
    ctx_refs, proj_refs = refs[:parts], refs[parts : 2 * parts]
    send_ref, keep_ref, full = refs[2 * parts :]
    rows = send_ref.shape[1]
    acc = begun_ref[...]
    for part in range(parts):
        acc = acc + dot(ctx_refs[part][...], proj_refs[part][...])
    full[...] = acc
    core = place[0]
    for far in range(2):
        gone = pl.multiple_of((far * 2 + 1 - core) * rows, rows)
        kept = pl.multiple_of((far * 2 + core) * rows, rows)
        send_ref[far] = full[pl.ds(gone, rows), :].astype(BF16)
        keep_ref[far] = full[pl.ds(kept, rows), :]


def project(core, contexts, projs):
    rows, width = contexts[0].shape
    cols = projs[0].shape[1]
    early, late = (0, 3), (1, 2)
    in_vmem = pl.BlockSpec(memory_space=pltpu.VMEM)
    in_any = pl.BlockSpec(memory_space=pl.ANY)
    begun, *late_projs = pl.pallas_call(
        begin_kernel,
        out_shape=(jax.ShapeDtypeStruct((rows, cols), F32),)
        + (jax.ShapeDtypeStruct((width, cols), BF16),) * len(late),
        in_specs=[in_vmem] * 4 + [in_any] * len(late),
        out_specs=(in_vmem,) * (1 + len(late)),
        scratch_shapes=[pltpu.SemaphoreType.DMA((len(late),))],
        cost_estimate=pl.CostEstimate(flops=5 * 10**8, bytes_accessed=2 * 10**6, transcendentals=0),
        compiler_params=pltpu.CompilerParams(vmem_limit_bytes=24 * 1024 * 1024),
        name="begin",
    )(
        *[contexts[part] for part in early],
        *[projs[part] for part in early],
        *[projs[part] for part in late],
    )
    return pl.pallas_call(
        project_kernel,
        out_shape=(
            jax.ShapeDtypeStruct((2, rows // 4, cols), BF16),
            jax.ShapeDtypeStruct((2, rows // 4, cols), F32),
        ),
        in_specs=[pl.BlockSpec(memory_space=pltpu.SMEM)] + [in_vmem] * 5,
        out_specs=(in_vmem, in_vmem),
        scratch_shapes=[pltpu.VMEM((rows, cols), F32)],
        cost_estimate=pl.CostEstimate(flops=5 * 10**8, bytes_accessed=2 * 10**6, transcendentals=0),
        compiler_params=pltpu.CompilerParams(vmem_limit_bytes=24 * 1024 * 1024),
        name="project",
    )(core, begun, *[contexts[part] for part in late], *late_projs)


def dispatch_kernel(place, near_ref, got_ref, slot_ref, own_ref, *refs):
    box_refs, resid_ref = refs[:-1], refs[-1]
    for far in range(2):
        residual = (near_ref[far].astype(F32) + got_ref[far].astype(F32)).astype(BF16)
        resid_ref[far] = residual
        for step, box_ref in enumerate(box_refs):
            index = step * 2 + far
            pick = one_hot(iota((CAP, residual.shape[0]), 0) == slot_ref[index : index + 1, :])
            box_ref[far] = dot(pick, residual).astype(BF16)
    own_ref[...] = resid_ref[place[0]]


def dispatch(far, near, got, slots):
    _, _, cols = near.shape
    steps = slots.shape[0] // 2
    in_vmem = pl.BlockSpec(memory_space=pltpu.VMEM)
    return pl.pallas_call(
        dispatch_kernel,
        out_shape=(jax.ShapeDtypeStruct(near.shape[1:], BF16),)
        + (jax.ShapeDtypeStruct((2, CAP, cols), BF16),) * steps,
        in_specs=[pl.BlockSpec(memory_space=pltpu.SMEM)] + [in_vmem] * 3,
        out_specs=(in_vmem,) * (1 + steps),
        scratch_shapes=[pltpu.VMEM(near.shape, BF16)],
        cost_estimate=pl.CostEstimate(flops=10**8, bytes_accessed=2 * 10**6, transcendentals=0),
        compiler_params=pltpu.CompilerParams(vmem_limit_bytes=8 * 1024 * 1024),
        name="dispatch",
    )(far, near, got, slots)


def hold_kernel(from_ref, _, held_ref, sems):
    pieces = sems.shape[0]
    rows = from_ref.shape[0] // pieces
    copies = [
        pltpu.make_async_copy(
            from_ref.at[pl.ds(piece * rows, rows)], held_ref.at[pl.ds(piece * rows, rows)], sems.at[piece]
        )
        for piece in range(pieces)
    ]
    for copy in copies:
        copy.start()
    for copy in copies:
        copy.wait()


def hold(weight, after, grant):
    in_vmem = pl.BlockSpec(memory_space=pltpu.VMEM)
    return pl.pallas_call(
        hold_kernel,
        out_shape=jax.ShapeDtypeStruct(weight.shape, weight.dtype),
        in_specs=[pl.BlockSpec(memory_space=pltpu.HBM), pl.BlockSpec(memory_space=pl.ANY)],
        out_specs=in_vmem,
        scratch_shapes=[pltpu.SemaphoreType.DMA((8,))],
        cost_estimate=pl.CostEstimate(flops=4 * 10**9, bytes_accessed=10**7, transcendentals=0),
        compiler_params=pltpu.CompilerParams(vmem_limit_bytes=grant * 1024 * 1024),
        name="hold",
    )(weight, after)


IN_COLS = 640


def expert_kernel(place, *refs):
    parts = 4
    row_refs = refs[: 2 * parts]
    gain_ref, router_ref, choose_ref, w_in, w_out, send_ref, hidden, gate_ref = refs[2 * parts : 2 * parts + 8]
    (rows_all,) = refs[2 * parts + 8 :]
    narrow_at, core = place[0], place[1]
    features, hidden_units = w_in.shape
    _, slots, quarter = row_refs[0].shape
    blocks = [lax.rem(narrow_at + parts - step, parts) for step in range(parts)]

    for which, side in ((0, core), (1, 1 - core)):
        for far in range(2):
            squares = jnp.zeros((slots, 1), F32)
            for part in range(parts):
                rows = row_refs[which * parts + part][far].astype(F32)
                squares = squares + jnp.sum(rows * rows, axis=1, keepdims=True)
            inverse = lax.rsqrt(squares / features + norm_eps)
            at = pl.multiple_of((far * 2 + side) * slots, 16)
            for part in range(parts):
                rows = row_refs[which * parts + part][far].astype(F32)
                normed = rows * inverse * gain_ref[blocks[part]]
                rows_all[part, pl.ds(at, slots), :] = normed.astype(BF16)
    logits = jnp.zeros((4 * slots, 3 * router_ref.shape[0]), F32)
    for part in range(parts):
        exact = router_ref[:, pl.ds(pl.multiple_of(blocks[part] * quarter, quarter), quarter)]
        high = exact.astype(BF16)
        rest = exact - high.astype(F32)
        middle = rest.astype(BF16)
        low = (rest - middle.astype(F32)).astype(BF16)
        pieces = jnp.concatenate([high.astype(F32), middle.astype(F32), low.astype(F32)], axis=0)
        logits = logits + lax.dot_general(
            rows_all[part],
            pieces.astype(BF16),
            (((1,), (1,)), ((), ())),
            preferred_element_type=F32,
        )
    differ = jnp.sum(logits * choose_ref[:, : logits.shape[1]], axis=1, keepdims=True)
    gate = 1.0 / (1.0 + jnp.exp(-differ))
    for step in range(hidden_units // IN_COLS):
        cols = slice(step * IN_COLS, (step + 1) * IN_COLS)
        acc = None
        for part in range(parts):
            at = pl.multiple_of(blocks[part] * quarter, quarter)
            term = dot(rows_all[part], w_in[pl.ds(at, quarter), cols])
            acc = term if acc is None else acc + term
        hidden[:, cols] = jax.nn.gelu(acc, approximate=True).astype(BF16)
    gate_ref[...] = jnp.broadcast_to(gate, gate_ref.shape)
    for far in range(2):
        at = pl.multiple_of((far * 2 + 1 - core) * quarter, quarter)
        send_ref[far] = (dot(hidden[...], w_out[:, pl.ds(at, quarter)]) * gate).astype(BF16)


def finish_kernel(place, hidden, gate_ref, w_out, keep_ref):
    quarter = keep_ref.shape[2]
    gate = gate_ref[:, :1]
    for far in range(2):
        at = pl.multiple_of((far * 2 + place[1]) * quarter, quarter)
        keep_ref[far] = dot(hidden[...], w_out[:, pl.ds(at, quarter)]) * gate


def finish(place, hidden, gate, w_out):
    in_vmem = pl.BlockSpec(memory_space=pltpu.VMEM)
    return pl.pallas_call(
        finish_kernel,
        out_shape=jax.ShapeDtypeStruct((2, hidden.shape[0], w_out.shape[1] // 4), F32),
        in_specs=[pl.BlockSpec(memory_space=pltpu.SMEM)] + [in_vmem] * 3,
        out_specs=in_vmem,
        cost_estimate=pl.CostEstimate(flops=10**9, bytes_accessed=8 * 10**6, transcendentals=0),
        compiler_params=pltpu.CompilerParams(vmem_limit_bytes=8 * 1024 * 1024),
        name="finish",
    )(place, hidden, gate, w_out)


def expert(place, own, other, gain, router, choose, w_in, w_out):
    _, slots, quarter = own[0].shape
    parts = len(own)
    rows = 4 * slots
    _, units = w_in.shape
    in_vmem = pl.BlockSpec(memory_space=pltpu.VMEM)
    return pl.pallas_call(
        expert_kernel,
        out_shape=(
            jax.ShapeDtypeStruct((2, rows, quarter), BF16),
            jax.ShapeDtypeStruct((rows, units), BF16),
            jax.ShapeDtypeStruct((rows, 128), F32),
        ),
        in_specs=[pl.BlockSpec(memory_space=pltpu.SMEM)]
        + [in_vmem] * (2 * parts + 5),
        out_specs=(in_vmem,) * 3,
        scratch_shapes=[
            pltpu.VMEM((parts, rows, quarter), BF16),
        ],
        cost_estimate=pl.CostEstimate(flops=4 * 10**9, bytes_accessed=24 * 10**6, transcendentals=10**5),
        compiler_params=pltpu.CompilerParams(vmem_limit_bytes=12 * 1024 * 1024),
        name="expert",
    )(place, *own, *other, gain, router, choose, w_in, w_out)


def share_kernel(place, keep_ref, got_ref, *box_refs):
    slots = box_refs[0].shape[1]
    for step, box_ref in enumerate(box_refs):
        block = lax.rem(place[0] + step, len(box_refs))
        at = pl.ds(pl.multiple_of(block * slots, 16), slots)
        for far in range(2):
            box_ref[far] = (keep_ref[far, at, :] + got_ref[far, at, :].astype(F32)).astype(BF16)


def share(place, keep, got, peers):
    _, rows, cols = keep.shape
    in_vmem = pl.BlockSpec(memory_space=pltpu.VMEM)
    return pl.pallas_call(
        share_kernel,
        out_shape=(jax.ShapeDtypeStruct((2, rows // peers, cols), BF16),) * peers,
        in_specs=[pl.BlockSpec(memory_space=pltpu.SMEM), in_vmem, in_vmem],
        out_specs=(in_vmem,) * peers,
        cost_estimate=pl.CostEstimate(flops=10**7, bytes_accessed=4 * 10**6, transcendentals=0),
        compiler_params=pltpu.CompilerParams(vmem_limit_bytes=8 * 1024 * 1024),
        name="share",
    )(place, keep, got)


def combine_kernel(place, slot_ref, resid_ref, *refs):
    box_refs, (send_ref, keep_ref, both) = refs[:-3], refs[-3:]
    tokens = slot_ref.shape[1]
    for far in range(2):
        acc = jnp.zeros(both.shape[1:], F32)
        for step, box_ref in enumerate(box_refs):
            pick = one_hot(iota((CAP, tokens), 0) == slot_ref[step : step + 1, :])
            acc = acc + lax.dot_general(
                pick, box_ref[far], (((0,), (0,)), ((), ())), preferred_element_type=F32
            )
        both[far] = acc
    send_ref[...] = both[1 - place[0]].astype(BF16)
    keep_ref[...] = both[place[0]] + resid_ref[...].astype(F32)


def combine(place, slots, resid, boxes):
    in_vmem = pl.BlockSpec(memory_space=pltpu.VMEM)
    return pl.pallas_call(
        combine_kernel,
        out_shape=(
            jax.ShapeDtypeStruct(resid.shape, BF16),
            jax.ShapeDtypeStruct(resid.shape, F32),
        ),
        in_specs=[pl.BlockSpec(memory_space=pltpu.SMEM)] + [in_vmem] * (2 + len(boxes)),
        out_specs=(in_vmem, in_vmem),
        scratch_shapes=[pltpu.VMEM((2, *resid.shape), F32)],
        cost_estimate=pl.CostEstimate(flops=10**8, bytes_accessed=2 * 10**6, transcendentals=0),
        compiler_params=pltpu.CompilerParams(vmem_limit_bytes=8 * 1024 * 1024),
        name="combine",
    )(place, slots, resid, *boxes)


def ring(count, step):
    return [(i, (i + step) % count) for i in range(count)]


def pick_at(values, index, axis=0):
    return lax.dynamic_index_in_dim(
        values, index, axis, keepdims=False, allow_negative_indices=False
    )


def body(
    hidden_in,
    queries,
    lang_ids,
    owner_slot,
    enc_kv,
    attn_proj,
    norm_gain,
    router_proj,
    expert_ids,
    proj_in,
    proj_out,
):
    narrow_count = lax.axis_size("narrow")
    depth_count = lax.axis_size("depth")
    wide_count = lax.axis_size("wide")
    tok_rows, quarter = hidden_in.shape
    seg_rows, _ = queries.shape
    experts = narrow_count
    peers = range(narrow_count)
    wide_at = lax.axis_index("wide")
    narrow_at = lax.axis_index("narrow")
    depth_at = lax.axis_index("depth")
    core, far = depth_at & 1, depth_at >> 1
    core_perm = [(i, i ^ 1) for i in range(depth_count)]
    far_perm = [(i, i ^ 2) for i in range(depth_count)]

    swap_perm = [
        (n * depth_count + d, d * narrow_count + n)
        for n in range(narrow_count)
        for d in range(depth_count)
    ]

    def around(values):
        return [values[0]] + [
            lax.ppermute(values[step], "narrow", ring(narrow_count, step))
            for step in peers
            if step
        ]

    def to_core(value):
        return lax.ppermute(value, "depth", core_perm)

    def to_far(value):
        return lax.ppermute(value, "depth", far_perm)

    last = narrow_count - 1
    around_to = [(narrow_at + step) & last for step in peers]

    def prepared(id_blocks):
        names = id_blocks[:, :, :, None] == jnp.arange(experts, dtype=jnp.int32)
        named = jnp.any(names, axis=2)
        ranks = jnp.where(named, jnp.cumsum(named.astype(jnp.int32), axis=1) - 1, -1)
        ranks = jnp.moveaxis(ranks, 2, 0)
        my_blocks = jnp.stack([core, 2 + core])
        around_from = (narrow_at - jnp.arange(narrow_count, dtype=jnp.int32)) & last
        send_slots = ranks[jnp.stack(around_to)][:, my_blocks].reshape(2 * narrow_count, tok_rows)
        get_slots = pick_at(ranks, narrow_at, 1)[around_from]
        my_ranks = pick_at(ranks, narrow_at)
        filled = my_ranks[:, None, :] == jnp.arange(CAP, dtype=jnp.int32)[None, :, None]
        here = jnp.arange(experts, dtype=jnp.int32) == narrow_at
        weigh = jnp.where(here[None, None, :], 1.0, -1.0) * named
        choose = jnp.sum(jnp.where(filled[:, :, :, None], weigh[:, None, :, :], 0.0), axis=2)
        choose = choose.reshape(-1, experts)
        choose = jnp.pad(jnp.concatenate([choose] * 3, axis=1), ((0, 0), (0, 128 - 3 * experts)))
        return tuple(
            with_layout_constraint(value, Layout(tuple(range(value.ndim))))
            for value in (send_slots, get_slots, choose)
        )

    def swapped(value):
        return lax.ppermute(value, ("narrow", "depth"), swap_perm)

    def spread():
        projs = around(
            [
                lax.dynamic_slice(
                    attn_proj,
                    (0, around_to[step] * quarter),
                    (attn_proj.shape[0], quarter),
                    allow_negative_indices=False,
                )
                for step in peers
            ],
        )
        return tuple(projs)

    def exchanged(boxes, attend_to, gathered):
        segment = lax.all_to_all(boxes, "wide", split_axis=0, concat_axis=0, tiled=True)
        projs = spread()
        partial, id_blocks, hidden = lax.optimization_barrier(
            (attend_to(segment), expert_ids.reshape(-1, tok_rows, 2), hidden_in)
        )
        returned = lax.all_to_all(partial, "wide", split_axis=0, concat_axis=0, tiled=True)
        returned, projs, hidden, ready = lax.optimization_barrier(
            (returned, projs, swapped(hidden), prepared(id_blocks))
        )
        return gathered(returned), projs, (hidden, *ready)

    def routed(boxes):
        return exchanged(
            boxes,
            lambda segment: attend_routed(counts, segment, enc_kv[0]),
            lambda returned: gather_rows(slots, returned),
        )

    def general(_):
        langs = lang_ids.reshape(wide_count, seg_rows)
        match = langs[:, :, None] == jnp.arange(owner_slot.shape[0], dtype=jnp.int32)
        holder = jnp.sum(jnp.where(match, owner_slot, 0), axis=2)
        return exchanged(
            jnp.broadcast_to(queries[None], (wide_count, *queries.shape)),
            lambda segment: attend(wide_at[None], holder, segment, enc_kv[0]),
            lambda returned: jnp.sum(returned, axis=0, dtype=BF16),
        )

    boxes, slots, counts, fits = route(wide_at[None], owner_slot, lang_ids, queries, wide_count)
    context, projs, ready = lax.cond(fits[0] == 1, routed, general, boxes)
    hidden_swapped, send_slots, get_slots, choose = ready
    contexts = around([context] * narrow_count)

    send, keep = project(core[None], contexts, projs)
    own_block = jnp.where(jnp.arange(2)[:, None, None] == far, hidden_swapped.astype(F32), 0.0)
    near = (keep + to_core(send).astype(F32) + own_block).astype(BF16)
    w_in = hold(proj_in[0], send, 2)
    got, w_in = lax.optimization_barrier((to_far(near), w_in))
    residual, *boxes = dispatch(far[None], near, got, send_slots)
    own_rows = around(boxes)
    w_out = hold(proj_out[0], residual, 2)
    own_resid = lax.ppermute(residual, ("narrow", "depth"), swap_perm)
    own_rows[1], w_out, own_resid = lax.optimization_barrier((own_rows[1], w_out, own_resid))
    other_rows = [to_core(part) for part in own_rows]

    place = jnp.stack([narrow_at, core])
    out_send, hidden, gate = expert(
        place,
        own_rows,
        other_rows,
        norm_gain.reshape(narrow_count, 1, quarter),
        router_proj.T,
        choose,
        w_in,
        w_out,
    )
    out_keep = finish(place, hidden, gate, w_out)
    arrived = around(share(narrow_at[None], out_keep, to_core(out_send), narrow_count))
    far_send, own_sum = combine(far[None], get_slots, own_resid, arrived)
    return (own_sum + to_far(far_send).astype(F32)).astype(BF16)


def solution(mesh):
    return jax.shard_map(
        body,
        mesh=mesh,
        in_specs=(
            P(("wide", "narrow"), "depth"),
            P("wide", ("narrow", "depth")),
            P(),
            P(),
            P("wide", None, None, ("narrow", "depth")),
            P(("narrow", "depth"), None),
            P(),
            P(),
            P("wide", None),
            P("narrow", None, "depth"),
            P("narrow", "depth", None),
        ),
        out_specs=P(("wide", "narrow"), "depth"),
        check_vma=False,
    )
```

```python
import jax
import jax.numpy as jnp
from jax import lax
from jax.experimental import pallas as pl
from jax.experimental.layout import Layout, with_layout_constraint
from jax.experimental.pallas import tpu as pltpu
from jax.sharding import PartitionSpec as P


HEAD_DIM = 64
CAP = 48
norm_eps = 1e-06
F32 = jnp.float32
BF16 = jnp.bfloat16
ROWS_BLOCK = 256


def dot(a, b):
    return jnp.dot(a, b, preferred_element_type=F32)


def iota(shape, dim):
    return lax.broadcasted_iota(jnp.int32, shape, dim)


def one_hot(flags):
    return jnp.where(flags, 1.0, 0.0).astype(BF16)


def attend_block(query, kv_ref):
    width = query.shape[1]
    head_of = iota((1, width), 1) // HEAD_DIM
    total = jnp.zeros(query.shape, F32)
    for head in range(width // HEAD_DIM):
        mine = head_of == head
        scores = lax.dot_general(
            jnp.where(mine, query, jnp.zeros_like(query)),
            kv_ref[0],
            (((1,), (1,)), ((), ())),
            preferred_element_type=F32,
        )
        weights = jnp.exp(scores - jnp.max(scores, axis=1, keepdims=True))
        norm = jnp.sum(weights, axis=1, keepdims=True)
        taken = dot(weights.astype(BF16), kv_ref[1])
        total = jnp.where(mine, taken / norm, total)
    return total


def attend_kernel(place, holder_ref, q_ref, kv_from, out_ref, kv_ref, attended, kv_sem):
    sources, rows, width = q_ref.shape
    wide_span = rows + 128
    kv_copy = pltpu.make_async_copy(kv_from, kv_ref, kv_sem)
    kv_copy.start()
    mine = holder_ref[...] == place[0]
    upto = one_hot(iota((rows, rows), 0) <= iota((rows, rows), 1))
    within = dot(one_hot(mine), upto)
    counts = within[:, rows - 1 :]
    begins = [jnp.int32(0)]
    before = jnp.zeros((sources, 1), F32)
    for source in range(sources):
        count = counts[source : source + 1, :]
        before = before + jnp.where(iota((sources, 1), 0) > source, count, 0.0)
        begins.append(begins[-1] + jnp.sum(count).astype(jnp.int32))
    pos = jnp.where(mine, within - 1.0 + before, -1.0)
    pos_row = pos.astype(jnp.int32)
    pos_col = pos.T.astype(jnp.int32)
    blocks = (begins[sources] + ROWS_BLOCK - 1) // ROWS_BLOCK
    rest = pl.ds(pl.multiple_of(blocks * ROWS_BLOCK, ROWS_BLOCK), wide_span)
    attended[rest, :] = jnp.zeros((wide_span, width), BF16)
    kv_copy.wait()

    def block(index, _):
        begin = pl.multiple_of(index * ROWS_BLOCK, ROWS_BLOCK)
        query = jnp.zeros((ROWS_BLOCK, width), F32)
        for source in range(sources):
            pick = one_hot(iota((ROWS_BLOCK, rows), 0) + begin == pos_row[source : source + 1, :])
            query = query + dot(pick, q_ref[source])
        total = attend_block((query * HEAD_DIM**-0.5).astype(BF16), kv_ref)
        attended[pl.ds(begin, ROWS_BLOCK), :] = total.astype(BF16)
        return 0

    lax.fori_loop(0, blocks, block, 0)
    for source in range(sources):
        at = pl.multiple_of((begins[source] // 16) * 16, 16)
        put = one_hot(iota((rows, wide_span), 1) + at == pos_col[:, source : source + 1])
        out_ref[source] = dot(put, attended[pl.ds(at, wide_span), :]).astype(BF16)


def attend(wide_at, holder, queries, keys_values):
    sources, rows, width = queries.shape
    capacity = sources * rows + rows + 128
    in_vmem = pl.BlockSpec(memory_space=pltpu.VMEM)
    return pl.pallas_call(
        attend_kernel,
        out_shape=jax.ShapeDtypeStruct(queries.shape, BF16),
        in_specs=[
            pl.BlockSpec(memory_space=pltpu.SMEM),
            in_vmem,
            in_vmem,
            pl.BlockSpec(memory_space=pl.ANY),
        ],
        out_specs=in_vmem,
        scratch_shapes=[
            pltpu.VMEM(keys_values.shape, BF16),
            pltpu.VMEM((capacity, width), BF16),
            pltpu.SemaphoreType.DMA,
        ],
        cost_estimate=pl.CostEstimate(flops=10**9, bytes_accessed=4 * 10**6, transcendentals=10**6),
        compiler_params=pltpu.CompilerParams(vmem_limit_bytes=32 * 1024 * 1024),
        name="attend",
    )(wide_at, holder, queries, keys_values)


ROUTE = 128


def route_kernel(place, slot_of, lang_ref, q_ref, box_ref, slot_ref, count_ref, fits_ref):
    sources, _, _ = box_ref.shape
    rows = q_ref.shape[0]
    langs = lang_ref[...]
    holder = jnp.zeros_like(langs)
    for lang in range(slot_of.shape[0]):
        holder = jnp.where(langs == lang, slot_of[lang], holder)
    pieces = langs.shape[0] // sources
    per_line = [
        jnp.sum(jnp.where(holder == which, 1.0, 0.0), axis=1, keepdims=True)
        for which in range(sources)
    ]
    per_line = jnp.concatenate(per_line, axis=1)
    join = one_hot(iota((sources, langs.shape[0]), 1) // pieces == iota((sources, langs.shape[0]), 0))
    counts = dot(join, per_line.astype(BF16))
    fits_ref[0] = (jnp.max(counts) <= ROUTE).astype(jnp.int32)
    here = jnp.sum(jnp.where(iota((1, sources), 1) == place[0], counts, 0.0), axis=1, keepdims=True)
    for source in range(sources):
        count_ref[source] = jnp.sum(here[source : source + 1, :]).astype(jnp.int32)
    line_of = iota(holder.shape, 0) - place[0] * pieces
    own = jnp.concatenate(
        [
            jnp.sum(jnp.where(line_of == piece, holder, 0), axis=0, keepdims=True)
            for piece in range(pieces)
        ],
        axis=1,
    )
    goes = own == iota((sources, rows), 0)
    upto = one_hot(iota((rows, rows), 0) <= iota((rows, rows), 1))
    slots = jnp.where(goes, dot(one_hot(goes), upto) - 1.0, -1.0).astype(jnp.int32)
    slot_ref[...] = slots
    for which in range(sources):
        pick = one_hot(iota((ROUTE, rows), 0) == slots[which : which + 1, :])
        box_ref[which] = dot(pick, q_ref[...]).astype(BF16)


def route(wide_at, owner_slot, lang_ids, queries, sources):
    rows, width = queries.shape
    in_vmem = pl.BlockSpec(memory_space=pltpu.VMEM)
    in_smem = pl.BlockSpec(memory_space=pltpu.SMEM)
    return pl.pallas_call(
        route_kernel,
        out_shape=(
            jax.ShapeDtypeStruct((sources, ROUTE, width), BF16),
            jax.ShapeDtypeStruct((sources, rows), jnp.int32),
            jax.ShapeDtypeStruct((sources,), jnp.int32),
            jax.ShapeDtypeStruct((1,), jnp.int32),
        ),
        in_specs=[in_smem, in_smem, in_vmem, in_vmem],
        out_specs=(in_vmem, in_vmem, in_smem, in_smem),
        cost_estimate=pl.CostEstimate(flops=10**8, bytes_accessed=10**6, transcendentals=0),
        compiler_params=pltpu.CompilerParams(vmem_limit_bytes=16 * 1024 * 1024),
        name="route",
    )(wide_at, owner_slot, lang_ids.reshape(-1, 128), queries)


def routed_kernel(counts, q_ref, kv_from, out_ref, kv_ref, lined, attended, kv_sem):
    sources, span, width = q_ref.shape
    kv_copy = pltpu.make_async_copy(kv_from, kv_ref, kv_sem)
    kv_copy.start()
    begins = [0]
    for source in range(sources):
        begins.append(begins[-1] + counts[source])
    blocks = (begins[sources] + ROWS_BLOCK - 1) // ROWS_BLOCK
    rest = pl.ds(pl.multiple_of(blocks * ROWS_BLOCK, ROWS_BLOCK), 2 * span)
    attended[rest, :] = jnp.zeros((2 * span, width), BF16)
    lane = iota((1, 2 * span), 1)
    ranks = []
    for source in range(0, sources, 2):
        first = jnp.where(lane < counts[source], begins[source] + lane, -1)
        second = jnp.where(lane - span < counts[source + 1], begins[source + 1] + lane - span, -1)
        ranks.append(jnp.where(lane < span, first, second))

    def pack(index, _):
        begin = pl.multiple_of(index * ROWS_BLOCK, ROWS_BLOCK)
        query = jnp.zeros((ROWS_BLOCK, width), F32)
        for pair, rank in enumerate(ranks):
            pick = one_hot(iota((ROWS_BLOCK, 2 * span), 0) + begin == rank)
            query = query + dot(pick, q_ref[2 * pair : 2 * pair + 2].reshape(2 * span, width))
        lined[pl.ds(begin, ROWS_BLOCK), :] = (query * HEAD_DIM**-0.5).astype(BF16)
        return 0

    lax.fori_loop(0, blocks, pack, 0)
    kv_copy.wait()

    def block(index, _):
        here = pl.ds(pl.multiple_of(index * ROWS_BLOCK, ROWS_BLOCK), ROWS_BLOCK)
        attended[here, :] = attend_block(lined[here, :], kv_ref).astype(BF16)
        return 0

    lax.fori_loop(0, blocks, block, 0)
    for source in range(sources):
        at = pl.multiple_of((begins[source] // 16) * 16, 16)
        shift = begins[source] - at
        put = one_hot(iota((span, 2 * span), 1) == iota((span, 2 * span), 0) + shift)
        out_ref[source] = dot(put, attended[pl.ds(at, 2 * span), :]).astype(BF16)


def attend_routed(counts, queries, keys_values):
    sources, span, width = queries.shape
    capacity = sources * span + 2 * ROWS_BLOCK
    in_vmem = pl.BlockSpec(memory_space=pltpu.VMEM)
    return pl.pallas_call(
        routed_kernel,
        out_shape=jax.ShapeDtypeStruct(queries.shape, BF16),
        in_specs=[
            pl.BlockSpec(memory_space=pltpu.SMEM),
            in_vmem,
            pl.BlockSpec(memory_space=pl.ANY),
        ],
        out_specs=in_vmem,
        scratch_shapes=[
            pltpu.VMEM(keys_values.shape, BF16),
            pltpu.VMEM((capacity, width), BF16),
            pltpu.VMEM((capacity, width), BF16),
            pltpu.SemaphoreType.DMA,
        ],
        cost_estimate=pl.CostEstimate(flops=10**9, bytes_accessed=4 * 10**6, transcendentals=10**6),
        compiler_params=pltpu.CompilerParams(vmem_limit_bytes=32 * 1024 * 1024),
        name="attend",
    )(counts, queries, keys_values)


def gather_kernel(slot_ref, box_ref, out_ref):
    sources, span, width = box_ref.shape
    rows = out_ref.shape[0]
    slot_col = slot_ref[...].astype(F32).T.astype(jnp.int32)
    total = jnp.zeros((rows, width), F32)
    for which in range(sources):
        pick = one_hot(iota((rows, span), 1) == slot_col[:, which : which + 1])
        total = total + dot(pick, box_ref[which])
    out_ref[...] = total.astype(BF16)


def gather_rows(slots, boxes):
    in_vmem = pl.BlockSpec(memory_space=pltpu.VMEM)
    return pl.pallas_call(
        gather_kernel,
        out_shape=jax.ShapeDtypeStruct((slots.shape[1], boxes.shape[2]), BF16),
        in_specs=[in_vmem, in_vmem],
        out_specs=in_vmem,
        cost_estimate=pl.CostEstimate(flops=10**8, bytes_accessed=10**6, transcendentals=0),
        compiler_params=pltpu.CompilerParams(vmem_limit_bytes=16 * 1024 * 1024),
        name="gather",
    )(slots, boxes)


def begin_kernel(*refs):
    parts = (len(refs) - 2) // 4
    late_from, late_to, sems = refs[2 * parts : 3 * parts], refs[3 * parts + 1 : 4 * parts + 1], refs[-1]
    copies = [
        pltpu.make_async_copy(late_from[part], late_to[part], sems.at[part]) for part in range(parts)
    ]
    for copy in copies:
        copy.start()
    acc = dot(refs[0][...], refs[parts][...])
    for part in range(1, parts):
        acc = acc + dot(refs[part][...], refs[parts + part][...])
    refs[3 * parts][...] = acc
    for copy in copies:
        copy.wait()


def project_kernel(place, begun_ref, *refs):
    parts = (len(refs) - 3) // 2
    ctx_refs, proj_refs = refs[:parts], refs[parts : 2 * parts]
    send_ref, keep_ref, full = refs[2 * parts :]
    rows = send_ref.shape[1]
    acc = begun_ref[...]
    for part in range(parts):
        acc = acc + dot(ctx_refs[part][...], proj_refs[part][...])
    full[...] = acc
    core = place[0]
    for far in range(2):
        gone = pl.multiple_of((far * 2 + 1 - core) * rows, rows)
        kept = pl.multiple_of((far * 2 + core) * rows, rows)
        send_ref[far] = full[pl.ds(gone, rows), :].astype(BF16)
        keep_ref[far] = full[pl.ds(kept, rows), :]


def project(core, contexts, projs):
    rows, width = contexts[0].shape
    cols = projs[0].shape[1]
    early, late = (0, 3), (1, 2)
    in_vmem = pl.BlockSpec(memory_space=pltpu.VMEM)
    in_any = pl.BlockSpec(memory_space=pl.ANY)
    begun, *late_projs = pl.pallas_call(
        begin_kernel,
        out_shape=(jax.ShapeDtypeStruct((rows, cols), F32),)
        + (jax.ShapeDtypeStruct((width, cols), BF16),) * len(late),
        in_specs=[in_vmem] * 4 + [in_any] * len(late),
        out_specs=(in_vmem,) * (1 + len(late)),
        scratch_shapes=[pltpu.SemaphoreType.DMA((len(late),))],
        cost_estimate=pl.CostEstimate(flops=5 * 10**8, bytes_accessed=2 * 10**6, transcendentals=0),
        compiler_params=pltpu.CompilerParams(vmem_limit_bytes=24 * 1024 * 1024),
        name="begin",
    )(
        *[contexts[part] for part in early],
        *[projs[part] for part in early],
        *[projs[part] for part in late],
    )
    return pl.pallas_call(
        project_kernel,
        out_shape=(
            jax.ShapeDtypeStruct((2, rows // 4, cols), BF16),
            jax.ShapeDtypeStruct((2, rows // 4, cols), F32),
        ),
        in_specs=[pl.BlockSpec(memory_space=pltpu.SMEM)] + [in_vmem] * 5,
        out_specs=(in_vmem, in_vmem),
        scratch_shapes=[pltpu.VMEM((rows, cols), F32)],
        cost_estimate=pl.CostEstimate(flops=5 * 10**8, bytes_accessed=2 * 10**6, transcendentals=0),
        compiler_params=pltpu.CompilerParams(vmem_limit_bytes=24 * 1024 * 1024),
        name="project",
    )(core, begun, *[contexts[part] for part in late], *late_projs)


def dispatch_kernel(place, near_ref, got_ref, slot_ref, own_ref, *refs):
    box_refs, resid_ref = refs[:-1], refs[-1]
    for far in range(2):
        residual = (near_ref[far].astype(F32) + got_ref[far].astype(F32)).astype(BF16)
        resid_ref[far] = residual
        for step, box_ref in enumerate(box_refs):
            index = step * 2 + far
            pick = one_hot(iota((CAP, residual.shape[0]), 0) == slot_ref[index : index + 1, :])
            box_ref[far] = dot(pick, residual).astype(BF16)
    own_ref[...] = resid_ref[place[0]]


def dispatch(far, near, got, slots):
    _, _, cols = near.shape
    steps = slots.shape[0] // 2
    in_vmem = pl.BlockSpec(memory_space=pltpu.VMEM)
    return pl.pallas_call(
        dispatch_kernel,
        out_shape=(jax.ShapeDtypeStruct(near.shape[1:], BF16),)
        + (jax.ShapeDtypeStruct((2, CAP, cols), BF16),) * steps,
        in_specs=[pl.BlockSpec(memory_space=pltpu.SMEM)] + [in_vmem] * 3,
        out_specs=(in_vmem,) * (1 + steps),
        scratch_shapes=[pltpu.VMEM(near.shape, BF16)],
        cost_estimate=pl.CostEstimate(flops=10**8, bytes_accessed=2 * 10**6, transcendentals=0),
        compiler_params=pltpu.CompilerParams(vmem_limit_bytes=8 * 1024 * 1024),
        name="dispatch",
    )(far, near, got, slots)


def hold_kernel(from_ref, _, held_ref, sems):
    pieces = sems.shape[0]
    rows = from_ref.shape[0] // pieces
    copies = [
        pltpu.make_async_copy(
            from_ref.at[pl.ds(piece * rows, rows)], held_ref.at[pl.ds(piece * rows, rows)], sems.at[piece]
        )
        for piece in range(pieces)
    ]
    for copy in copies:
        copy.start()
    for copy in copies:
        copy.wait()


def hold(weight, after, grant):
    in_vmem = pl.BlockSpec(memory_space=pltpu.VMEM)
    return pl.pallas_call(
        hold_kernel,
        out_shape=jax.ShapeDtypeStruct(weight.shape, weight.dtype),
        in_specs=[pl.BlockSpec(memory_space=pltpu.HBM), pl.BlockSpec(memory_space=pl.ANY)],
        out_specs=in_vmem,
        scratch_shapes=[pltpu.SemaphoreType.DMA((8,))],
        cost_estimate=pl.CostEstimate(flops=4 * 10**9, bytes_accessed=10**7, transcendentals=0),
        compiler_params=pltpu.CompilerParams(vmem_limit_bytes=grant * 1024 * 1024),
        name="hold",
    )(weight, after)


IN_COLS = 640


def expert_kernel(place, *refs):
    parts = 4
    row_refs = refs[: 2 * parts]
    gain_ref, router_ref, choose_ref, w_in, w_out, send_ref, hidden, gate_ref = refs[2 * parts : 2 * parts + 8]
    (rows_all,) = refs[2 * parts + 8 :]
    narrow_at, core = place[0], place[1]
    features, hidden_units = w_in.shape
    _, slots, quarter = row_refs[0].shape
    blocks = [lax.rem(narrow_at + parts - step, parts) for step in range(parts)]

    for which, side in ((0, core), (1, 1 - core)):
        for far in range(2):
            squares = jnp.zeros((slots, 1), F32)
            for part in range(parts):
                rows = row_refs[which * parts + part][far].astype(F32)
                squares = squares + jnp.sum(rows * rows, axis=1, keepdims=True)
            inverse = lax.rsqrt(squares / features + norm_eps)
            at = pl.multiple_of((far * 2 + side) * slots, 16)
            for part in range(parts):
                rows = row_refs[which * parts + part][far].astype(F32)
                normed = rows * inverse * gain_ref[blocks[part]]
                rows_all[part, pl.ds(at, slots), :] = normed.astype(BF16)
    logits = jnp.zeros((4 * slots, 3 * router_ref.shape[0]), F32)
    for part in range(parts):
        exact = router_ref[:, pl.ds(pl.multiple_of(blocks[part] * quarter, quarter), quarter)]
        high = exact.astype(BF16)
        rest = exact - high.astype(F32)
        middle = rest.astype(BF16)
        low = (rest - middle.astype(F32)).astype(BF16)
        pieces = jnp.concatenate([high.astype(F32), middle.astype(F32), low.astype(F32)], axis=0)
        logits = logits + lax.dot_general(
            rows_all[part],
            pieces.astype(BF16),
            (((1,), (1,)), ((), ())),
            preferred_element_type=F32,
        )
    differ = jnp.sum(logits * choose_ref[:, : logits.shape[1]], axis=1, keepdims=True)
    gate = 1.0 / (1.0 + jnp.exp(-differ))
    for step in range(hidden_units // IN_COLS):
        cols = slice(step * IN_COLS, (step + 1) * IN_COLS)
        acc = None
        for part in range(parts):
            at = pl.multiple_of(blocks[part] * quarter, quarter)
            term = dot(rows_all[part], w_in[pl.ds(at, quarter), cols])
            acc = term if acc is None else acc + term
        hidden[:, cols] = jax.nn.gelu(acc, approximate=True).astype(BF16)
    gate_ref[...] = jnp.broadcast_to(gate, gate_ref.shape)
    for far in range(2):
        at = pl.multiple_of((far * 2 + 1 - core) * quarter, quarter)
        send_ref[far] = (dot(hidden[...], w_out[:, pl.ds(at, quarter)]) * gate).astype(BF16)


def finish_kernel(place, hidden, gate_ref, w_out, keep_ref):
    quarter = keep_ref.shape[2]
    gate = gate_ref[:, :1]
    for far in range(2):
        at = pl.multiple_of((far * 2 + place[1]) * quarter, quarter)
        keep_ref[far] = dot(hidden[...], w_out[:, pl.ds(at, quarter)]) * gate


def finish(place, hidden, gate, w_out):
    in_vmem = pl.BlockSpec(memory_space=pltpu.VMEM)
    return pl.pallas_call(
        finish_kernel,
        out_shape=jax.ShapeDtypeStruct((2, hidden.shape[0], w_out.shape[1] // 4), F32),
        in_specs=[pl.BlockSpec(memory_space=pltpu.SMEM)] + [in_vmem] * 3,
        out_specs=in_vmem,
        cost_estimate=pl.CostEstimate(flops=10**9, bytes_accessed=8 * 10**6, transcendentals=0),
        compiler_params=pltpu.CompilerParams(vmem_limit_bytes=8 * 1024 * 1024),
        name="finish",
    )(place, hidden, gate, w_out)


def expert(place, own, other, gain, router, choose, w_in, w_out):
    _, slots, quarter = own[0].shape
    parts = len(own)
    rows = 4 * slots
    _, units = w_in.shape
    in_vmem = pl.BlockSpec(memory_space=pltpu.VMEM)
    return pl.pallas_call(
        expert_kernel,
        out_shape=(
            jax.ShapeDtypeStruct((2, rows, quarter), BF16),
            jax.ShapeDtypeStruct((rows, units), BF16),
            jax.ShapeDtypeStruct((rows, 128), F32),
        ),
        in_specs=[pl.BlockSpec(memory_space=pltpu.SMEM)]
        + [in_vmem] * (2 * parts + 5),
        out_specs=(in_vmem,) * 3,
        scratch_shapes=[
            pltpu.VMEM((parts, rows, quarter), BF16),
        ],
        cost_estimate=pl.CostEstimate(flops=4 * 10**9, bytes_accessed=24 * 10**6, transcendentals=10**5),
        compiler_params=pltpu.CompilerParams(vmem_limit_bytes=12 * 1024 * 1024),
        name="expert",
    )(place, *own, *other, gain, router, choose, w_in, w_out)


def share_kernel(place, keep_ref, got_ref, *box_refs):
    slots = box_refs[0].shape[1]
    for step, box_ref in enumerate(box_refs):
        block = lax.rem(place[0] + step, len(box_refs))
        at = pl.ds(pl.multiple_of(block * slots, 16), slots)
        for far in range(2):
            box_ref[far] = (keep_ref[far, at, :] + got_ref[far, at, :].astype(F32)).astype(BF16)


def share(place, keep, got, peers):
    _, rows, cols = keep.shape
    in_vmem = pl.BlockSpec(memory_space=pltpu.VMEM)
    return pl.pallas_call(
        share_kernel,
        out_shape=(jax.ShapeDtypeStruct((2, rows // peers, cols), BF16),) * peers,
        in_specs=[pl.BlockSpec(memory_space=pltpu.SMEM), in_vmem, in_vmem],
        out_specs=(in_vmem,) * peers,
        cost_estimate=pl.CostEstimate(flops=10**7, bytes_accessed=4 * 10**6, transcendentals=0),
        compiler_params=pltpu.CompilerParams(vmem_limit_bytes=8 * 1024 * 1024),
        name="share",
    )(place, keep, got)


def combine_kernel(place, slot_ref, resid_ref, *refs):
    box_refs, (send_ref, keep_ref, both) = refs[:-3], refs[-3:]
    tokens = slot_ref.shape[1]
    for far in range(2):
        acc = jnp.zeros(both.shape[1:], F32)
        for step, box_ref in enumerate(box_refs):
            pick = one_hot(iota((CAP, tokens), 0) == slot_ref[step : step + 1, :])
            acc = acc + lax.dot_general(
                pick, box_ref[far], (((0,), (0,)), ((), ())), preferred_element_type=F32
            )
        both[far] = acc
    send_ref[...] = both[1 - place[0]].astype(BF16)
    keep_ref[...] = both[place[0]] + resid_ref[...].astype(F32)


def combine(place, slots, resid, boxes):
    in_vmem = pl.BlockSpec(memory_space=pltpu.VMEM)
    return pl.pallas_call(
        combine_kernel,
        out_shape=(
            jax.ShapeDtypeStruct(resid.shape, BF16),
            jax.ShapeDtypeStruct(resid.shape, F32),
        ),
        in_specs=[pl.BlockSpec(memory_space=pltpu.SMEM)] + [in_vmem] * (2 + len(boxes)),
        out_specs=(in_vmem, in_vmem),
        scratch_shapes=[pltpu.VMEM((2, *resid.shape), F32)],
        cost_estimate=pl.CostEstimate(flops=10**8, bytes_accessed=2 * 10**6, transcendentals=0),
        compiler_params=pltpu.CompilerParams(vmem_limit_bytes=8 * 1024 * 1024),
        name="combine",
    )(place, slots, resid, *boxes)


def ring(count, step):
    return [(i, (i + step) % count) for i in range(count)]


def pick_at(values, index, axis=0):
    return lax.dynamic_index_in_dim(
        values, index, axis, keepdims=False, allow_negative_indices=False
    )


def body(
    hidden_in,
    queries,
    lang_ids,
    owner_slot,
    enc_kv,
    attn_proj,
    norm_gain,
    router_proj,
    expert_ids,
    proj_in,
    proj_out,
):
    narrow_count = lax.axis_size("narrow")
    depth_count = lax.axis_size("depth")
    wide_count = lax.axis_size("wide")
    tok_rows, quarter = hidden_in.shape
    seg_rows, _ = queries.shape
    experts = narrow_count
    peers = range(narrow_count)
    wide_at = lax.axis_index("wide")
    narrow_at = lax.axis_index("narrow")
    depth_at = lax.axis_index("depth")
    core, far = depth_at & 1, depth_at >> 1
    core_perm = [(i, i ^ 1) for i in range(depth_count)]
    far_perm = [(i, i ^ 2) for i in range(depth_count)]

    swap_perm = [
        (n * depth_count + d, d * narrow_count + n)
        for n in range(narrow_count)
        for d in range(depth_count)
    ]

    def around(values):
        return [values[0]] + [
            lax.ppermute(values[step], "narrow", ring(narrow_count, step))
            for step in peers
            if step
        ]

    def to_core(value):
        return lax.ppermute(value, "depth", core_perm)

    def to_far(value):
        return lax.ppermute(value, "depth", far_perm)

    last = narrow_count - 1
    around_to = [(narrow_at + step) & last for step in peers]

    def prepared(id_blocks):
        names = id_blocks[:, :, :, None] == jnp.arange(experts, dtype=jnp.int32)
        named = jnp.any(names, axis=2)
        ranks = jnp.where(named, jnp.cumsum(named.astype(jnp.int32), axis=1) - 1, -1)
        ranks = jnp.moveaxis(ranks, 2, 0)
        my_blocks = jnp.stack([core, 2 + core])
        around_from = (narrow_at - jnp.arange(narrow_count, dtype=jnp.int32)) & last
        send_slots = ranks[jnp.stack(around_to)][:, my_blocks].reshape(2 * narrow_count, tok_rows)
        get_slots = pick_at(ranks, narrow_at, 1)[around_from]
        my_ranks = pick_at(ranks, narrow_at)
        filled = my_ranks[:, None, :] == jnp.arange(CAP, dtype=jnp.int32)[None, :, None]
        here = jnp.arange(experts, dtype=jnp.int32) == narrow_at
        weigh = jnp.where(here[None, None, :], 1.0, -1.0) * named
        choose = jnp.sum(jnp.where(filled[:, :, :, None], weigh[:, None, :, :], 0.0), axis=2)
        choose = choose.reshape(-1, experts)
        choose = jnp.pad(jnp.concatenate([choose] * 3, axis=1), ((0, 0), (0, 128 - 3 * experts)))
        return tuple(
            with_layout_constraint(value, Layout(tuple(range(value.ndim))))
            for value in (send_slots, get_slots, choose)
        )

    def swapped(value):
        return lax.ppermute(value, ("narrow", "depth"), swap_perm)

    def spread():
        projs = around(
            [
                lax.dynamic_slice(
                    attn_proj,
                    (0, around_to[step] * quarter),
                    (attn_proj.shape[0], quarter),
                    allow_negative_indices=False,
                )
                for step in peers
            ],
        )
        return tuple(projs)

    def exchanged(boxes, attend_to, gathered):
        segment = lax.all_to_all(boxes, "wide", split_axis=0, concat_axis=0, tiled=True)
        projs = spread()
        partial, id_blocks, hidden = lax.optimization_barrier(
            (attend_to(segment), expert_ids.reshape(-1, tok_rows, 2), hidden_in)
        )
        returned = lax.all_to_all(partial, "wide", split_axis=0, concat_axis=0, tiled=True)
        returned, projs, hidden, ready = lax.optimization_barrier(
            (returned, projs, swapped(hidden), prepared(id_blocks))
        )
        return gathered(returned), projs, (hidden, *ready)

    def routed(boxes):
        return exchanged(
            boxes,
            lambda segment: attend_routed(counts, segment, enc_kv[0]),
            lambda returned: gather_rows(slots, returned),
        )

    def general(_):
        langs = lang_ids.reshape(wide_count, seg_rows)
        match = langs[:, :, None] == jnp.arange(owner_slot.shape[0], dtype=jnp.int32)
        holder = jnp.sum(jnp.where(match, owner_slot, 0), axis=2)
        return exchanged(
            jnp.broadcast_to(queries[None], (wide_count, *queries.shape)),
            lambda segment: attend(wide_at[None], holder, segment, enc_kv[0]),
            lambda returned: jnp.sum(returned, axis=0, dtype=BF16),
        )

    boxes, slots, counts, fits = route(wide_at[None], owner_slot, lang_ids, queries, wide_count)
    context, projs, ready = lax.cond(fits[0] == 1, routed, general, boxes)
    hidden_swapped, send_slots, get_slots, choose = ready
    contexts = around([context] * narrow_count)

    send, keep = project(core[None], contexts, projs)
    own_block = jnp.where(jnp.arange(2)[:, None, None] == far, hidden_swapped.astype(F32), 0.0)
    near = (keep + to_core(send).astype(F32) + own_block).astype(BF16)
    w_in = hold(proj_in[0], send, 2)
    got, w_in = lax.optimization_barrier((to_far(near), w_in))
    residual, *boxes = dispatch(far[None], near, got, send_slots)
    own_rows = around(boxes)
    w_out = hold(proj_out[0], residual, 2)
    own_resid = lax.ppermute(residual, ("narrow", "depth"), swap_perm)
    own_rows[1], w_out, own_resid = lax.optimization_barrier((own_rows[1], w_out, own_resid))
    other_rows = [to_core(part) for part in own_rows]

    place = jnp.stack([narrow_at, core])
    out_send, hidden, gate = expert(
        place,
        own_rows,
        other_rows,
        norm_gain.reshape(narrow_count, 1, quarter),
        router_proj.T,
        choose,
        w_in,
        w_out,
    )
    out_keep = finish(place, hidden, gate, w_out)
    arrived = around(share(narrow_at[None], out_keep, to_core(out_send), narrow_count))
    far_send, own_sum = combine(far[None], get_slots, own_resid, arrived)
    return (own_sum + to_far(far_send).astype(F32)).astype(BF16)


def solution(mesh):
    return jax.shard_map(
        body,
        mesh=mesh,
        in_specs=(
            P(("wide", "narrow"), "depth"),
            P("wide", ("narrow", "depth")),
            P(),
            P(),
            P("wide", None, None, ("narrow", "depth")),
            P(("narrow", "depth"), None),
            P(),
            P(),
            P("wide", None),
            P("narrow", None, "depth"),
            P("narrow", "depth", None),
        ),
        out_specs=P(("wide", "narrow"), "depth"),
        check_vma=False,
    )
```
